32 devices in a mesh: src: 4 (over y, x), tgt: 8 (over z, core).
Axes of the slice: x: 2, y: 2, z: 4, core: 2. Of those that a mesh axis runs over, the one named last changes fastest.
Arguments:
- source_feats: bfloat16 [1, 16, 32, 1024], P(None, 'src', None, 'tgt'), may hold values from -200 to 200
- target_feats: bfloat16 [1, 32, 32, 1024], P(None, 'tgt', None, 'src'), may hold values from -200 to 200
- conv_one: bfloat16 [3, 3, 3, 3, 1, 16], replicated, may hold values from -1 to 1
- bias_one: float32 [16], replicated, may hold values from -1.5 to 1.5
- conv_two: bfloat16 [3, 3, 3, 3, 16, 16], replicated, may hold values from -0.25 to 0.25
- bias_two: float32 [16], replicated, may hold values from -1.5 to 1.5
- conv_three: bfloat16 [3, 3, 3, 3, 16, 1], replicated, may hold values from -0.25 to 0.25
- bias_three: float32 [1], replicated, may hold values from -1.5 to 1.5
Outputs:
- scores: bfloat16 [1, 16, 32, 32, 32], P(None, 'src', 'tgt')
The draws below stay inside these ranges and needn't reach their ends.
All inputs are finite; a program needn't handle non-finite values.
Results may differ from the reference program's by a relative error of at most 0.0049.
The reference program's roundings to bfloat16 on the way count: a program that leaves them out, or rounds other values in their place, can miss the bound.
Values may be sent and summed in bfloat16 or wider, within the bound.
No kernel may reach another device: no remote copies, remote signals or barrier semaphores. Data moves between devices by JAX's collectives and lax.ppermute only.
A program may use at most 256 MiB of HBM per device.

```python
import jax
import jax.numpy as jnp
from jax import lax

C = 1024
CH = 16
WA = 32
WB = 32
PAIRS = 1
HA = 16
HB = 32


def feature_draw(key, rows, cols, salt):
    protos = jax.random.normal(jax.random.fold_in(key, 7), (8, C), jnp.float32)
    own_key = jax.random.fold_in(key, salt)
    labels = jax.random.randint(jax.random.fold_in(own_key, 1), (PAIRS, rows, cols), 0, 8)
    onehot = (labels[..., None] == jnp.arange(8, dtype=jnp.int32)).astype(jnp.float32)
    mixed = jnp.einsum('pijk,kc->pijc', onehot, protos)
    noise = jax.random.normal(jax.random.fold_in(own_key, 2), (PAIRS, rows, cols, C), jnp.float32)
    channel_scale = 10.0 ** (jnp.arange(C, dtype=jnp.float32) / C)
    values = (1.2 * mixed + noise) * channel_scale
    return jnp.clip(values, -200.0, 200.0).astype(jnp.bfloat16)


def draw_source_feats(key, part):
    return feature_draw(key, HA, WA, 11)


def draw_target_feats(key, part):
    return feature_draw(key, HB, WB, 23)


def centred(stream_key, dims, spread, bound, held_as=jnp.bfloat16):
    drawn = spread * jax.random.normal(stream_key, dims, jnp.float32)
    return jnp.clip(drawn, min=-bound, max=bound).astype(held_as)


def setup_inputs(seed: int = 0) -> dict:
    arg_keys = jax.random.split(jax.random.key(seed), 9)
    return {
        "source_feats": draw_source_feats(jax.random.fold_in(arg_keys[8], 71), 0),
        "target_feats": draw_target_feats(jax.random.fold_in(arg_keys[8], 71), 0),
        "conv_one": centred(arg_keys[2], (3, 3, 3, 3, 1, CH), 40 ** -0.5, 1.0),
        "bias_one": centred(arg_keys[3], (CH,), 0.3, 1.5, jnp.float32),
        "conv_two": centred(arg_keys[4], (3, 3, 3, 3, CH, CH), (40 * CH) ** -0.5, 0.25),
        "bias_two": centred(arg_keys[5], (CH,), 0.3, 1.5, jnp.float32),
        "conv_three": centred(arg_keys[6], (3, 3, 3, 3, CH, 1), (40 * CH) ** -0.5, 0.25),
        "bias_three": centred(arg_keys[7], (1,), 0.5, 1.5, jnp.float32),
    }


epsilon = 1e-06

def normalize(feats):
    values = feats.astype(jnp.float32)
    squares = lax.optimization_barrier(jnp.sum(values * values, axis=-1, keepdims=True))
    return (values * lax.rsqrt(squares + epsilon)).astype(jnp.bfloat16)

def layer_ref(volume, kernel, biases):
    cout = kernel.shape[-1]
    padded = jnp.pad(volume, ((0, 0), (1, 1), (1, 1), (1, 1), (1, 1)))
    summed = jnp.zeros((cout, HA, WA, HB, WB), jnp.float32)
    for row_step in range(3):
        for col_step in range(3):
            for tgt_step in range(3):
                for lane_step in range(3):
                    piece = padded[:, row_step:row_step + HA, col_step:col_step + WA, tgt_step:tgt_step + HB, lane_step:lane_step + WB]
                    tap = kernel[row_step, col_step, tgt_step, lane_step].astype(jnp.float32)
                    summed = summed + jnp.einsum('aijkl,ab->bijkl', piece.astype(jnp.float32), tap)
    return jax.nn.relu(summed + biases[:, None, None, None, None]).astype(jnp.bfloat16)

def reference(source_feats, target_feats, conv_one, bias_one, conv_two, bias_two, conv_three, bias_three):

    def one_pair(pair):
        source_part, target_part = pair
        left = normalize(source_part).reshape(HA * WA, C)
        right = normalize(target_part).reshape(HB * WB, C)
        volume = jnp.dot(left, right.T, preferred_element_type=jnp.float32).astype(jnp.bfloat16)
        volume = volume.reshape(1, HA, WA, HB, WB)
        volume = layer_ref(volume, conv_one, bias_one)
        volume = layer_ref(volume, conv_two, bias_two)
        volume = layer_ref(volume, conv_three, bias_three)
        return jnp.transpose(volume[0], (0, 2, 1, 3))
    return lax.map(one_pair, (source_feats, target_feats))
```

```python
from functools import partial

import jax
import jax.numpy as jnp
from jax import lax
from jax.experimental import pallas as pl
from jax.experimental.pallas import tpu as pltpu
from jax.sharding import PartitionSpec as P

LANES = 128
TAPS = 3
HALO = 3
epsilon = 1e-06


def xor_blocks(block, axis):
    count = lax.axis_size(axis)
    blocks = block[None]
    step = 1
    while step < count:
        swap = [(i, i ^ step) for i in range(count)]
        blocks = jnp.concatenate([blocks, lax.ppermute(blocks, axis, swap)], axis=0)
        step *= 2
    return blocks


def cyclic_halo(block, axis, dim, width):
    count = lax.axis_size(axis)
    size = block.shape[dim]
    forward = [(i, (i + 1) % count) for i in range(count)]
    backward = [((i + 1) % count, i) for i in range(count)]
    low = lax.ppermute(lax.slice_in_dim(block, size - width, size, axis=dim), axis, forward)
    high = lax.ppermute(lax.slice_in_dim(block, 0, width, axis=dim), axis, backward)
    return jnp.concatenate([low, block, high], axis=dim)


def wide_blocks(blocks, axis):
    count, rows, chunk = blocks.shape
    if chunk % LANES == 0:
        return blocks, lax.axis_index(axis)
    order = lax.axis_index(axis) ^ jnp.arange(count)
    joined = jnp.take(blocks, order, axis=0).transpose(1, 0, 2).reshape(1, rows, count * chunk)
    return joined, jnp.int32(0)


def volume_kernel(pos_ref, src_ref, tgt_ref, out_ref, left_s, right_s, *, src_cols, tgt_cols):
    def normed(blocks_ref, held, index):
        count = blocks_ref.shape[0]
        squares = None
        for m in range(count):
            values = blocks_ref[m].astype(jnp.float32)
            part = jnp.sum(values * values, axis=-1, keepdims=True)
            squares = part if squares is None else squares + part
        scale = lax.rsqrt(squares + epsilon)
        for m in range(count):
            values = blocks_ref[m].astype(jnp.float32)
            held[index ^ m] = (values * scale).astype(jnp.bfloat16)
        return jnp.concatenate([held[m] for m in range(count)], axis=1)

    left = normed(src_ref, left_s, pos_ref[0])
    right = normed(tgt_ref, right_s, pos_ref[1])
    volume = lax.dot_general(
        left, right, (((1,), (1,)), ((), ())), preferred_element_type=jnp.float32
    )
    blocks = LANES // tgt_cols
    inner = src_cols // blocks
    for i in range(out_ref.shape[0]):
        for k in range(out_ref.shape[1]):
            pieces = [
                volume[
                    i * src_cols + b * inner : i * src_cols + (b + 1) * inner,
                    k * tgt_cols : (k + 1) * tgt_cols,
                ]
                for b in range(blocks)
            ]
            out_ref[i, k] = jnp.concatenate(pieces, axis=1).astype(jnp.bfloat16)


def weights_kernel(one_ref, two_ref, three_ref, w1_ref, w2_ref, w3_ref, w3_s, *, inner, rows_a, rows_b):
    channels = one_ref.shape[1]
    per_row = LANES // channels
    lane = lax.broadcasted_iota(jnp.int32, (channels, LANES), 1)
    row = lax.broadcasted_iota(jnp.int32, (channels, LANES), 0)
    lane_block = lane // channels
    spread = (lane % channels == row).astype(jnp.bfloat16)

    def tiled(ref):
        return jnp.dot(ref[...], spread, preferred_element_type=jnp.float32)

    def tap(a, b, e, g):
        return ((a * TAPS + b) * TAPS + e) * TAPS + g

    one = tiled(one_ref)
    column = jnp.where(row < inner, row, jnp.where(row == inner, inner, -2))
    column = jnp.where(row == 2 * inner - 1, -1, column)
    slabs = []
    for a in range(TAPS):
        for e in range(TAPS):
            for g in range(TAPS):
                slab = jnp.zeros((channels, LANES), jnp.float32)
                for b in range(TAPS):
                    n = tap(a, b, e, g)
                    hit = (column - lane_block == b - 1) & (column >= -1)
                    slab = jnp.where(hit, one[n : n + 1], slab)
                slabs.append(slab)
    while (len(slabs) * channels) % LANES:
        slabs.append(jnp.zeros((channels, LANES), jnp.float32))
    w1_ref[...] = jnp.concatenate(slabs, axis=0).T.astype(jnp.bfloat16)

    two = tiled(two_ref)
    for b in range(TAPS):
        for half in range(2):
            col = (b * 2 + half) * LANES
            for g in range(TAPS):
                for oi in range(2):
                    for ok in range(2):
                        block = jnp.zeros((channels, LANES), jnp.float32)
                        for low in range(2):
                            a = half * 2 + low - oi
                            if not 0 <= a < TAPS:
                                continue
                            for e in range(TAPS):
                                n = tap(a, b, e, g) * channels
                                hit = lane_block == low * 4 + ok + e
                                block = jnp.where(hit, two[n : n + channels], block)
                        at = ((g * 2 + oi) * 2 + ok) * channels
                        w2_ref[at : at + channels, col : col + LANES] = block.astype(jnp.bfloat16)

    three = tiled(three_ref)
    w3_s[...] = jnp.zeros_like(w3_s)
    lane_k = lax.broadcasted_iota(jnp.int32, (rows_b, LANES), 1) // channels
    row_k = lax.broadcasted_iota(jnp.int32, (rows_b, LANES), 0)
    for a in range(TAPS):
        for b in range(TAPS):
            for g in range(TAPS):
                block = jnp.zeros((rows_b, LANES), jnp.float32)
                for e in range(TAPS):
                    n = tap(a, b, e, g)
                    block = jnp.where(lane_k - row_k == e, three[n : n + 1], block)
                for oi in range(rows_a):
                    col = (b * (rows_a + 2) + oi + a) * LANES
                    at = (g * rows_a + oi) * rows_b
                    w3_s[at : at + rows_b, col : col + LANES] = block
    w3_ref[...] = w3_s[...].astype(jnp.bfloat16)


def layers_kernel(
    pos_ref, b3_ref, vol_ref, w1_ref, w2_ref, w3_ref, b1_ref, b2_ref, out_ref, vj, a1, a2,
    *, tgt_cols, inner, channels,
):
    ext_a, ext_b = vol_ref.shape[0], vol_ref.shape[1]
    first_a, count_a, first_b, count_b = pos_ref[0], pos_ref[1], pos_ref[2], pos_ref[3]
    wide = inner * LANES

    def inside(a, b, edge):
        ga = first_a + a - edge
        gb = first_b + b - edge
        return (ga >= 0) & (ga < count_a) & (gb >= 0) & (gb < count_b)

    def lanes(rows):
        return lax.broadcasted_iota(jnp.int32, (rows, LANES), 1)

    def up(x, step, unit, size):
        pos = lanes(x.shape[0]) % size
        return jnp.where(pos >= step, pltpu.roll(x, step, 1), 0.0)

    def down(x, step, unit, size):
        pos = lanes(x.shape[0]) % size
        return jnp.where(pos < size - step, pltpu.roll(x, LANES - step, 1), 0.0)

    plane_row = lax.broadcasted_iota(jnp.int32, (inner, LANES), 0)

    def spread_row(a, carry):
        for b in range(ext_b):
            x = vol_ref[a, b].astype(jnp.float32)
            x = jnp.where(inside(a, b, HALO), x, 0.0)
            before = up(x, tgt_cols, 0, LANES)
            after = down(x, tgt_cols, 0, LANES)
            edge = jnp.where(plane_row == inner - 1, before, jnp.where(plane_row == 0, after, 0.0))
            both = jnp.concatenate([x, edge], axis=0)
            rows = 2 * inner
            vj[a, b, 0:rows] = up(both, 1, 0, tgt_cols).astype(jnp.bfloat16)
            vj[a, b, rows : 2 * rows] = both.astype(jnp.bfloat16)
            vj[a, b, 2 * rows : 3 * rows] = down(both, 1, 0, tgt_cols).astype(jnp.bfloat16)
        return carry

    lax.fori_loop(0, ext_a, spread_row, 0)

    def put(dst, a, b, blocks):
        dst[a, b, 0:channels] = up(blocks[-1], tgt_cols, 0, LANES).astype(jnp.bfloat16)
        for n, block in enumerate(blocks):
            dst[a, b, (n + 1) * channels : (n + 2) * channels] = block.astype(jnp.bfloat16)
        dst[a, b, (inner + 1) * channels :] = down(blocks[0], tgt_cols, 0, LANES).astype(jnp.bfloat16)

    l1_a, l1_b = ext_a - 2, ext_b - 2
    bias1 = jnp.broadcast_to(b1_ref[...], (channels, LANES))
    depth1 = TAPS * TAPS * TAPS * 2 * inner
    group = 4 if l1_b % 4 == 0 else 2

    def first_row(a, carry):
        for b0 in range(0, l1_b, group):
            x = jnp.concatenate(
                [
                    jnp.concatenate(
                        [vj[a + da, b0 + n + db] for da in range(TAPS) for db in range(TAPS)], axis=0
                    )
                    for n in range(group)
                ],
                axis=1,
            )
            got = jnp.dot(w1_ref[:, :depth1], x, preferred_element_type=jnp.float32)
            for n in range(group):
                ok = inside(a, b0 + n, HALO - 1)
                blocks = [
                    jnp.where(
                        ok,
                        jnp.maximum(
                            got[c * channels : (c + 1) * channels, n * LANES : (n + 1) * LANES]
                            + bias1,
                            0.0,
                        ),
                        0.0,
                    )
                    for c in range(inner)
                ]
                put(a1, a, b0 + n, blocks)
        return carry

    lax.fori_loop(0, l1_a, first_row, 0)

    l2_a, l2_b = l1_a - 2, l1_b - 2
    bias2 = jnp.broadcast_to(b2_ref[...], (channels, LANES))
    cells = 4 * channels
    half = inner // 2

    for a in range(l2_a):
        for b in range(l2_b, a2.shape[1]):
            a2[a, b] = jnp.zeros(a2.shape[2:], jnp.bfloat16)

    def second_patch(n, carry):
        pa = (n // (l2_b // 2)) * 2
        pb = (n % (l2_b // 2)) * 2
        for h in range(2):
            x = jnp.concatenate(
                [
                    jnp.concatenate(
                        [
                            a1[pa + wi, pb + wk, (c + dj) * channels : (c + dj + 1) * channels]
                            for dj in range(TAPS)
                            for wi in range(4)
                            for wk in range(4)
                        ],
                        axis=0,
                    )
                    for c in range(h * half, (h + 1) * half)
                ],
                axis=1,
            )
            got = jnp.dot(w2_ref[...], x, preferred_element_type=jnp.float32)
            for q in range(half):
                part = got[:, q * LANES : (q + 1) * LANES]
                total = (
                    part[cells : 2 * cells]
                    + up(part[:cells], 1, 0, tgt_cols)
                    + down(part[2 * cells :], 1, 0, tgt_cols)
                )
                c = h * half + q
                for oi in range(2):
                    for ok in range(2):
                        at = (oi * 2 + ok) * channels
                        block = jnp.maximum(total[at : at + channels] + bias2, 0.0)
                        block = jnp.where(inside(pa + oi, pb + ok, HALO - 2), block, 0.0)
                        a2[pa + oi, pb + ok, (c + 1) * channels : (c + 2) * channels] = block.astype(
                            jnp.bfloat16
                        )
                        if c == inner - 1:
                            a2[pa + oi, pb + ok, 0:channels] = up(block, tgt_cols, 0, LANES).astype(
                                jnp.bfloat16
                            )
                        if c == 0:
                            a2[pa + oi, pb + ok, (inner + 1) * channels :] = down(
                                block, tgt_cols, 0, LANES
                            ).astype(jnp.bfloat16)
        return carry

    lax.fori_loop(0, (l2_a // 2) * (l2_b // 2), second_patch, 0)

    cells = out_ref.shape[0]
    for h in range(2):
        x = jnp.concatenate(
            [
                jnp.concatenate(
                    [
                        a2[wi, wk, (c + dj) * channels : (c + dj + 1) * channels]
                        for dj in range(TAPS)
                        for wi in range(l2_a)
                        for wk in range(a2.shape[1])
                    ],
                    axis=0,
                )
                for c in range(h * half, (h + 1) * half)
            ],
            axis=1,
        )
        got = jnp.dot(w3_ref[...], x, preferred_element_type=jnp.float32)
        for q in range(half):
            part = got[:, q * LANES : (q + 1) * LANES]
            total = (
                part[cells : 2 * cells]
                + up(part[:cells], 1, 0, tgt_cols)
                + down(part[2 * cells :], 1, 0, tgt_cols)
            )
            c = h * half + q
            out_ref[:, c * LANES : (c + 1) * LANES] = jnp.maximum(total + b3_ref[0], 0.0).astype(
                jnp.bfloat16
            )


VMEM = pl.BlockSpec(memory_space=pltpu.VMEM)
SMEM = pl.BlockSpec(memory_space=pltpu.SMEM)


def one_pair(source, target, conv_one, bias_one, conv_two, bias_two, conv_three, bias_three):
    rows_a, src_cols, _ = source.shape
    rows_b, tgt_cols, _ = target.shape
    channels = conv_two.shape[-1]
    blocks = LANES // tgt_cols
    inner = src_cols // blocks
    assert 2 * inner == channels and LANES % tgt_cols == 0
    assert rows_a % 2 == 0 and rows_b % 2 == 0 and min(rows_a, rows_b) >= HALO

    left = xor_blocks(source.reshape(rows_a * src_cols, -1), "tgt")
    right = xor_blocks(target.reshape(rows_b * tgt_cols, -1), "src")
    left, left_at = wide_blocks(left, "tgt")
    right, right_at = wide_blocks(right, "src")

    taps = TAPS**4
    w3_cols = TAPS * (rows_a + 2) * LANES
    w1_cols = -(-(TAPS**3 * channels) // LANES) * LANES
    w1, w2, w3 = pl.pallas_call(
        partial(weights_kernel, inner=inner, rows_a=rows_a, rows_b=rows_b),
        out_shape=(
            jax.ShapeDtypeStruct((LANES, w1_cols), jnp.bfloat16),
            jax.ShapeDtypeStruct((TAPS * 4 * channels, TAPS * 2 * LANES), jnp.bfloat16),
            jax.ShapeDtypeStruct((TAPS * rows_a * rows_b, w3_cols), jnp.bfloat16),
        ),
        in_specs=[VMEM] * 3,
        out_specs=(VMEM, VMEM, VMEM),
        scratch_shapes=[pltpu.VMEM((TAPS * rows_a * rows_b, w3_cols), jnp.float32)],
        cost_estimate=pl.CostEstimate(flops=2_000_000_000, bytes_accessed=1_000_000, transcendentals=0),
        name="weights",
    )(
        conv_one.reshape(taps, channels),
        conv_two.reshape(taps, channels, channels).swapaxes(1, 2).reshape(taps * channels, channels),
        conv_three.reshape(taps, channels),
    )

    volume = pl.pallas_call(
        partial(volume_kernel, src_cols=src_cols, tgt_cols=tgt_cols),
        out_shape=jax.ShapeDtypeStruct((rows_a, rows_b, inner, LANES), jnp.bfloat16),
        in_specs=[SMEM, VMEM, VMEM],
        out_specs=VMEM,
        scratch_shapes=[pltpu.VMEM(left.shape, jnp.bfloat16), pltpu.VMEM(right.shape, jnp.bfloat16)],
        name="volume",
    )(jnp.stack([left_at, right_at]).astype(jnp.int32), left, right)

    volume = cyclic_halo(volume, "src", 0, HALO)
    volume = cyclic_halo(volume, "tgt", 1, HALO)
    ext_a, ext_b = rows_a + 2 * HALO, rows_b + 2 * HALO
    place = jnp.stack(
        [
            lax.axis_index("src") * rows_a,
            lax.axis_size("src") * rows_a,
            lax.axis_index("tgt") * rows_b,
            lax.axis_size("tgt") * rows_b,
        ]
    ).astype(jnp.int32)
    wide_b = LANES // channels
    scores = pl.pallas_call(
        partial(layers_kernel, tgt_cols=tgt_cols, inner=inner, channels=channels),
        out_shape=jax.ShapeDtypeStruct((rows_a * rows_b, inner * LANES), jnp.bfloat16),
        in_specs=[SMEM, SMEM] + [VMEM] * 6,
        out_specs=VMEM,
        scratch_shapes=[
            pltpu.VMEM((ext_a, ext_b, TAPS * 2 * inner, LANES), jnp.bfloat16),
            pltpu.VMEM((ext_a - 2, ext_b - 2, (inner + 2) * channels, LANES), jnp.bfloat16),
            pltpu.VMEM((ext_a - 4, wide_b, (inner + 2) * channels, LANES), jnp.bfloat16),
        ],
        name="layers",
    )(place, bias_three, volume, w1, w2, w3, bias_one[:, None], bias_two[:, None])
    scores = scores.reshape(rows_a, rows_b, inner, blocks, tgt_cols).transpose(0, 1, 3, 2, 4)
    return scores.reshape(rows_a, rows_b, src_cols, tgt_cols)


def local(source_feats, target_feats, *params):
    return jnp.stack(
        [one_pair(source_feats[p], target_feats[p], *params) for p in range(source_feats.shape[0])]
    )


def solution(mesh):
    return jax.shard_map(
        local,
        mesh=mesh,
        in_specs=(
            P(None, "src", None, "tgt"),
            P(None, "tgt", None, "src"),
            P(),
            P(),
            P(),
            P(),
            P(),
            P(),
        ),
        out_specs=P(None, "src", "tgt", None, None),
        check_vma=False,
    )
```

```python
from functools import partial

import jax
import jax.numpy as jnp
from jax import lax
from jax.experimental import pallas as pl
from jax.experimental.pallas import tpu as pltpu
from jax.sharding import PartitionSpec as P

LANES = 128
TAPS = 3
HALO = 3
epsilon = 1e-06


def xor_blocks(block, axis):
    count = lax.axis_size(axis)
    held, masks = block[None], [0]
    pieces, piece_masks = [held], [[0]]
    step = count // 2
    while step:
        swap = [(i, i ^ step) for i in range(count)]
        got = lax.ppermute(held, axis, swap)
        got_masks = [m ^ step for m in masks]
        pieces.append(got)
        piece_masks.append(got_masks)
        masks = masks + got_masks
        if step > 1:
            held = jnp.concatenate([held, got], axis=0)
        step //= 2
    return pieces, piece_masks


def swap_edges(low_edge, high_edge, axis):
    count = lax.axis_size(axis)
    forward = [(i, (i + 1) % count) for i in range(count)]
    backward = [((i + 1) % count, i) for i in range(count)]
    return lax.ppermute(high_edge, axis, forward), lax.ppermute(low_edge, axis, backward)


def wide_blocks(pieces, masks, axis):
    chunk = pieces[0].shape[-1]
    if chunk % LANES == 0:
        return pieces, masks, axis
    flat = [m for group in masks for m in group]
    blocks = jnp.concatenate(pieces, axis=0)
    place = [flat.index(m) for m in range(len(flat))]
    order = jnp.asarray(place, jnp.int32)[lax.axis_index(axis) ^ jnp.arange(len(flat))]
    joined = jnp.take(blocks, order, axis=0).transpose(1, 0, 2)
    return [joined.reshape(1, joined.shape[0], -1)], [[0]], None


def volume_kernel(*refs, masks, axes, src_cols, tgt_cols):
    counts = [len(group) for group in masks]
    left_refs, right_refs = refs[: counts[0]], refs[counts[0] : sum(counts)]
    out_ref, low_ref, high_ref, left_s, right_s = refs[sum(counts) :]

    def normed(block_refs, block_masks, axis, held):
        where = [(ref, n, m) for ref, group in zip(block_refs, block_masks) for n, m in enumerate(group)]
        squares = None
        for ref, n, _ in where:
            values = ref[n].astype(jnp.float32)
            part = jnp.sum(values * values, axis=-1, keepdims=True)
            squares = part if squares is None else squares + part
        scale = lax.rsqrt(squares + epsilon)
        index = 0 if axis is None else lax.axis_index(axis)
        for ref, n, m in where:
            held[index ^ m] = (ref[n].astype(jnp.float32) * scale).astype(jnp.bfloat16)
        return jnp.concatenate([held[n] for n in range(len(where))], axis=1)

    left = normed(left_refs, masks[0], axes[0], left_s)
    right = normed(right_refs, masks[1], axes[1], right_s)
    volume = lax.dot_general(
        left, right, (((1,), (1,)), ((), ())), preferred_element_type=jnp.float32
    )
    blocks = LANES // tgt_cols
    inner = src_cols // blocks
    rows_a = out_ref.shape[0]
    for i in range(rows_a):
        for k in range(out_ref.shape[1]):
            pieces = [
                volume[
                    i * src_cols + b * inner : i * src_cols + (b + 1) * inner,
                    k * tgt_cols : (k + 1) * tgt_cols,
                ]
                for b in range(blocks)
            ]
            plane = jnp.concatenate(pieces, axis=1).astype(jnp.bfloat16)
            out_ref[i, k] = plane
            if i < HALO:
                low_ref[i, k] = plane
            if i >= rows_a - HALO:
                high_ref[i - rows_a + HALO, k] = plane


def weights_kernel(one_ref, two_ref, three_ref, w1_ref, w2_ref, w3_ref, w3_s, *, inner, rows_a, rows_b):
    channels = one_ref.shape[1]
    per_row = LANES // channels
    lane = lax.broadcasted_iota(jnp.int32, (channels, LANES), 1)
    row = lax.broadcasted_iota(jnp.int32, (channels, LANES), 0)
    lane_block = lane // channels
    spread = (lane % channels == row).astype(jnp.bfloat16)

    def tiled(ref):
        return jnp.dot(ref[...], spread, preferred_element_type=jnp.float32)

    def tap(a, b, e, g):
        return ((a * TAPS + b) * TAPS + e) * TAPS + g

    one = tiled(one_ref)
    column = jnp.where(row < inner, row, jnp.where(row == inner, inner, -2))
    column = jnp.where(row == 2 * inner - 1, -1, column)
    slabs = []
    for a in range(TAPS):
        for e in range(TAPS):
            for g in range(TAPS):
                slab = jnp.zeros((channels, LANES), jnp.float32)
                for b in range(TAPS):
                    n = tap(a, b, e, g)
                    hit = (column - lane_block == b - 1) & (column >= -1)
                    slab = jnp.where(hit, one[n : n + 1], slab)
                slabs.append(slab)
    while (len(slabs) * channels) % LANES:
        slabs.append(jnp.zeros((channels, LANES), jnp.float32))
    w1_ref[...] = jnp.concatenate(slabs, axis=0).T.astype(jnp.bfloat16)

    two = tiled(two_ref)
    for b in range(TAPS):
        for half in range(2):
            col = (b * 2 + half) * LANES
            for g in range(TAPS):
                for oi in range(2):
                    for ok in range(2):
                        block = jnp.zeros((channels, LANES), jnp.float32)
                        for low in range(2):
                            a = half * 2 + low - oi
                            if not 0 <= a < TAPS:
                                continue
                            for e in range(TAPS):
                                n = tap(a, b, e, g) * channels
                                hit = lane_block == low * 4 + ok + e
                                block = jnp.where(hit, two[n : n + channels], block)
                        at = ((g * 2 + oi) * 2 + ok) * channels
                        w2_ref[at : at + channels, col : col + LANES] = block.astype(jnp.bfloat16)

    three = tiled(three_ref)
    w3_s[...] = jnp.zeros_like(w3_s)
    lane_k = lax.broadcasted_iota(jnp.int32, (rows_b, LANES), 1) // channels
    row_k = lax.broadcasted_iota(jnp.int32, (rows_b, LANES), 0)
    for a in range(TAPS):
        for b in range(TAPS):
            for g in range(TAPS):
                block = jnp.zeros((rows_b, LANES), jnp.float32)
                for e in range(TAPS):
                    n = tap(a, b, e, g)
                    block = jnp.where(lane_k - row_k == e, three[n : n + 1], block)
                for oi in range(rows_a):
                    col = (b * (rows_a + 2) + oi + a) * LANES
                    at = (g * rows_a + oi) * rows_b
                    w3_s[at : at + rows_b, col : col + LANES] = block
    w3_ref[...] = w3_s[...].astype(jnp.bfloat16)


def layers_kernel(
    b1_ref, b2_ref, b3_ref, own_ref, low_a_ref, high_a_ref, low_b_ref, high_b_ref,
    w1_ref, w2_ref, w3_ref, out_ref, vj, a1, a2, *, sizes, tgt_cols, inner, channels,
):
    rows_a, rows_b = own_ref.shape[0], own_ref.shape[1]
    ext_a, ext_b = rows_a + 2 * HALO, rows_b + 2 * HALO
    count_a, count_b = sizes[0] * rows_a, sizes[1] * rows_b
    first_a = lax.axis_index("src") * rows_a
    first_b = lax.axis_index("tgt") * rows_b

    def plane(a, b):
        if b < HALO:
            return low_b_ref[a, b]
        if b >= HALO + rows_b:
            return high_b_ref[a, b - HALO - rows_b]
        if a < HALO:
            return low_a_ref[a, b - HALO]
        if a >= HALO + rows_a:
            return high_a_ref[a - HALO - rows_a, b - HALO]
        return own_ref[a - HALO, b - HALO]

    def biases(ref):
        row = lax.broadcasted_iota(jnp.int32, (channels, LANES), 0)
        got = jnp.zeros((channels, LANES), jnp.float32)
        for c in range(channels):
            got = jnp.where(row == c, ref[c], got)
        return got

    def inside(a, b, edge):
        ga = first_a + a - edge
        gb = first_b + b - edge
        return (ga >= 0) & (ga < count_a) & (gb >= 0) & (gb < count_b)

    def lanes(rows):
        return lax.broadcasted_iota(jnp.int32, (rows, LANES), 1)

    def up(x, step, unit, size):
        pos = lanes(x.shape[0]) % size
        return jnp.where(pos >= step, pltpu.roll(x, step, 1), 0.0)

    def down(x, step, unit, size):
        pos = lanes(x.shape[0]) % size
        return jnp.where(pos < size - step, pltpu.roll(x, LANES - step, 1), 0.0)

    plane_row = lax.broadcasted_iota(jnp.int32, (inner, LANES), 0)

    def spread_row(a):
        for b in range(ext_b):
            x = plane(a, b).astype(jnp.float32)
            x = jnp.where(inside(a, b, HALO), x, 0.0)
            before = up(x, tgt_cols, 0, LANES)
            after = down(x, tgt_cols, 0, LANES)
            edge = jnp.where(plane_row == inner - 1, before, jnp.where(plane_row == 0, after, 0.0))
            both = jnp.concatenate([x, edge], axis=0)
            rows = 2 * inner
            vj[a, b, 0:rows] = up(both, 1, 0, tgt_cols).astype(jnp.bfloat16)
            vj[a, b, rows : 2 * rows] = both.astype(jnp.bfloat16)
            vj[a, b, 2 * rows : 3 * rows] = down(both, 1, 0, tgt_cols).astype(jnp.bfloat16)

    for a in range(ext_a):
        spread_row(a)

    def put(dst, a, b, blocks):
        dst[a, b, 0:channels] = up(blocks[-1], tgt_cols, 0, LANES).astype(jnp.bfloat16)
        for n, block in enumerate(blocks):
            dst[a, b, (n + 1) * channels : (n + 2) * channels] = block.astype(jnp.bfloat16)
        dst[a, b, (inner + 1) * channels :] = down(blocks[0], tgt_cols, 0, LANES).astype(jnp.bfloat16)

    l1_a, l1_b = ext_a - 2, ext_b - 2
    bias1 = biases(b1_ref)
    depth1 = TAPS * TAPS * TAPS * 2 * inner
    group = 4 if l1_b % 4 == 0 else 2

    def first_row(a):
        for b0 in range(0, l1_b, group):
            x = jnp.concatenate(
                [
                    jnp.concatenate(
                        [vj[a + da, b0 + n + db] for da in range(TAPS) for db in range(TAPS)], axis=0
                    )
                    for n in range(group)
                ],
                axis=1,
            )
            got = jnp.dot(w1_ref[:, :depth1], x, preferred_element_type=jnp.float32)
            for n in range(group):
                ok = inside(a, b0 + n, HALO - 1)
                blocks = [
                    jnp.where(
                        ok,
                        jnp.maximum(
                            got[c * channels : (c + 1) * channels, n * LANES : (n + 1) * LANES]
                            + bias1,
                            0.0,
                        ),
                        0.0,
                    )
                    for c in range(inner)
                ]
                put(a1, a, b0 + n, blocks)

    for a in range(l1_a):
        first_row(a)

    l2_a, l2_b = l1_a - 2, l1_b - 2
    bias2 = biases(b2_ref)
    cells = 4 * channels
    half = inner // 2

    for a in range(l2_a):
        for b in range(l2_b, a2.shape[1]):
            a2[a, b] = jnp.zeros(a2.shape[2:], jnp.bfloat16)

    def second_patch(pa, pb):
        for h in range(2):
            x = jnp.concatenate(
                [
                    jnp.concatenate(
                        [
                            a1[pa + wi, pb + wk, (c + dj) * channels : (c + dj + 1) * channels]
                            for dj in range(TAPS)
                            for wi in range(4)
                            for wk in range(4)
                        ],
                        axis=0,
                    )
                    for c in range(h * half, (h + 1) * half)
                ],
                axis=1,
            )
            got = jnp.dot(w2_ref[...], x, preferred_element_type=jnp.float32)
            for q in range(half):
                part = got[:, q * LANES : (q + 1) * LANES]
                total = (
                    part[cells : 2 * cells]
                    + up(part[:cells], 1, 0, tgt_cols)
                    + down(part[2 * cells :], 1, 0, tgt_cols)
                )
                c = h * half + q
                for oi in range(2):
                    for ok in range(2):
                        at = (oi * 2 + ok) * channels
                        block = jnp.maximum(total[at : at + channels] + bias2, 0.0)
                        block = jnp.where(inside(pa + oi, pb + ok, HALO - 2), block, 0.0)
                        a2[pa + oi, pb + ok, (c + 1) * channels : (c + 2) * channels] = block.astype(
                            jnp.bfloat16
                        )
                        if c == inner - 1:
                            a2[pa + oi, pb + ok, 0:channels] = up(block, tgt_cols, 0, LANES).astype(
                                jnp.bfloat16
                            )
                        if c == 0:
                            a2[pa + oi, pb + ok, (inner + 1) * channels :] = down(
                                block, tgt_cols, 0, LANES
                            ).astype(jnp.bfloat16)

    for pa in range(0, l2_a, 2):
        for pb in range(0, l2_b, 2):
            second_patch(pa, pb)

    cells = rows_a * rows_b
    columns = []
    for h in range(2):
        x = jnp.concatenate(
            [
                jnp.concatenate(
                    [
                        a2[wi, wk, (c + dj) * channels : (c + dj + 1) * channels]
                        for dj in range(TAPS)
                        for wi in range(l2_a)
                        for wk in range(a2.shape[1])
                    ],
                    axis=0,
                )
                for c in range(h * half, (h + 1) * half)
            ],
            axis=1,
        )
        got = jnp.dot(w3_ref[...], x, preferred_element_type=jnp.float32)
        for q in range(half):
            part = got[:, q * LANES : (q + 1) * LANES]
            total = (
                part[cells : 2 * cells]
                + up(part[:cells], 1, 0, tgt_cols)
                + down(part[2 * cells :], 1, 0, tgt_cols)
            )
            columns.append(jnp.maximum(total + b3_ref[0], 0.0))
    scores = jnp.stack(columns, axis=0).swapaxes(0, 1)
    for n in range(cells):
        for b in range(LANES // tgt_cols):
            out_ref[n // rows_b, n % rows_b, b * inner : (b + 1) * inner] = scores[
                n, :, b * tgt_cols : (b + 1) * tgt_cols
            ].astype(jnp.bfloat16)


VMEM = pl.BlockSpec(memory_space=pltpu.VMEM)
SMEM = pl.BlockSpec(memory_space=pltpu.SMEM)


def one_pair(source, target, conv_one, bias_one, conv_two, bias_two, conv_three, bias_three):
    rows_a, src_cols, _ = source.shape
    rows_b, tgt_cols, _ = target.shape
    channels = conv_two.shape[-1]
    blocks = LANES // tgt_cols
    inner = src_cols // blocks
    assert 2 * inner == channels and LANES % tgt_cols == 0
    assert rows_a % 2 == 0 and rows_b % 2 == 0 and min(rows_a, rows_b) >= HALO

    left, left_masks = xor_blocks(source.reshape(rows_a * src_cols, -1), "tgt")
    right, right_masks = xor_blocks(target.reshape(rows_b * tgt_cols, -1), "src")
    left, left_masks, left_axis = wide_blocks(left, left_masks, "tgt")
    right, right_masks, right_axis = wide_blocks(right, right_masks, "src")

    taps = TAPS**4
    w3_cols = TAPS * (rows_a + 2) * LANES
    w1_cols = -(-(TAPS**3 * channels) // LANES) * LANES
    w1, w2, w3 = pl.pallas_call(
        partial(weights_kernel, inner=inner, rows_a=rows_a, rows_b=rows_b),
        out_shape=(
            jax.ShapeDtypeStruct((LANES, w1_cols), jnp.bfloat16),
            jax.ShapeDtypeStruct((TAPS * 4 * channels, TAPS * 2 * LANES), jnp.bfloat16),
            jax.ShapeDtypeStruct((TAPS * rows_a * rows_b, w3_cols), jnp.bfloat16),
        ),
        in_specs=[VMEM] * 3,
        out_specs=(VMEM, VMEM, VMEM),
        scratch_shapes=[pltpu.VMEM((TAPS * rows_a * rows_b, w3_cols), jnp.float32)],
        cost_estimate=pl.CostEstimate(flops=2_000_000_000, bytes_accessed=1_000_000, transcendentals=0),
        compiler_params=pltpu.CompilerParams(vmem_limit_bytes=8 << 20),
        name="weights",
    )(
        conv_one.reshape(taps, channels),
        conv_two.reshape(taps, channels, channels).swapaxes(1, 2).reshape(taps * channels, channels),
        conv_three.reshape(taps, channels),
    )

    def held(pieces):
        return pltpu.VMEM((sum(p.shape[0] for p in pieces), *pieces[0].shape[1:]), jnp.bfloat16)

    edge = jax.ShapeDtypeStruct((HALO, rows_b, inner, LANES), jnp.bfloat16)
    own, low_edge, high_edge = pl.pallas_call(
        partial(
            volume_kernel,
            masks=(left_masks, right_masks),
            axes=(left_axis, right_axis),
            src_cols=src_cols,
            tgt_cols=tgt_cols,
        ),
        out_shape=(jax.ShapeDtypeStruct((rows_a, rows_b, inner, LANES), jnp.bfloat16), edge, edge),
        in_specs=[VMEM] * (len(left) + len(right)),
        out_specs=(VMEM,) * 3,
        scratch_shapes=[held(left), held(right)],
        compiler_params=pltpu.CompilerParams(vmem_limit_bytes=8 << 20),
        name="volume",
    )(*left, *right)

    low_a, high_a = swap_edges(low_edge, high_edge, "src")
    tall = [low_a, own, high_a]
    low_edge = jnp.concatenate([x[:, :HALO] for x in tall], axis=0)
    high_edge = jnp.concatenate([x[:, rows_b - HALO :] for x in tall], axis=0)
    low_b, high_b = swap_edges(low_edge, high_edge, "tgt")
    ext_a, ext_b = rows_a + 2 * HALO, rows_b + 2 * HALO
    return pl.pallas_call(
        partial(
            layers_kernel,
            sizes=(lax.axis_size("src"), lax.axis_size("tgt")),
            tgt_cols=tgt_cols,
            inner=inner,
            channels=channels,
        ),
        out_shape=jax.ShapeDtypeStruct((rows_a, rows_b, src_cols, tgt_cols), jnp.bfloat16),
        in_specs=[SMEM] * 3 + [VMEM] * 8,
        out_specs=VMEM,
        scratch_shapes=[
            pltpu.VMEM((ext_a, ext_b, TAPS * 2 * inner, LANES), jnp.bfloat16),
            pltpu.VMEM((ext_a - 2, ext_b - 2, (inner + 2) * channels, LANES), jnp.bfloat16),
            pltpu.VMEM((ext_a - 4, LANES // channels, (inner + 2) * channels, LANES), jnp.bfloat16),
        ],
        compiler_params=pltpu.CompilerParams(vmem_limit_bytes=20 << 20),
        name="layers",
    )(bias_one, bias_two, bias_three, own, low_a, high_a, low_b, high_b, w1, w2, w3)


def local(source_feats, target_feats, *params):
    return jnp.stack(
        [one_pair(source_feats[p], target_feats[p], *params) for p in range(source_feats.shape[0])]
    )


def solution(mesh):
    return jax.shard_map(
        local,
        mesh=mesh,
        in_specs=(
            P(None, "src", None, "tgt"),
            P(None, "tgt", None, "src"),
            P(),
            P(),
            P(),
            P(),
            P(),
            P(),
        ),
        out_specs=P(None, "src", "tgt", None, None),
        check_vma=False,
    )
```

```python
from functools import partial

import jax
import jax.numpy as jnp
from jax import lax
from jax.experimental import pallas as pl
from jax.experimental.pallas import tpu as pltpu
from jax.sharding import PartitionSpec as P

LANES = 128
TAPS = 3
HALO = 3
epsilon = 1e-06


def xor_blocks(block, axis):
    count = lax.axis_size(axis)
    held, masks = block[None], [0]
    pieces, piece_masks = [held], [[0]]
    step = count // 2
    while step:
        swap = [(i, i ^ step) for i in range(count)]
        got = lax.ppermute(held, axis, swap)
        got_masks = [m ^ step for m in masks]
        pieces.append(got)
        piece_masks.append(got_masks)
        masks = masks + got_masks
        if step > 1:
            held = jnp.concatenate([held, got], axis=0)
        step //= 2
    return pieces, piece_masks


def swap_edges(low_edge, high_edge, axis):
    count = lax.axis_size(axis)
    forward = [(i, (i + 1) % count) for i in range(count)]
    backward = [((i + 1) % count, i) for i in range(count)]
    return lax.ppermute(high_edge, axis, forward), lax.ppermute(low_edge, axis, backward)


def wide_blocks(pieces, masks, axis):
    chunk = pieces[0].shape[-1]
    if chunk % LANES == 0:
        return pieces, masks, axis
    flat = [m for group in masks for m in group]
    blocks = jnp.concatenate(pieces, axis=0)
    place = [flat.index(m) for m in range(len(flat))]
    order = jnp.asarray(place, jnp.int32)[lax.axis_index(axis) ^ jnp.arange(len(flat))]
    joined = jnp.take(blocks, order, axis=0).transpose(1, 0, 2)
    return [joined.reshape(1, joined.shape[0], -1)], [[0]], None


def volume_kernel(*refs, masks, axes, src_cols, tgt_cols):
    counts = [len(group) for group in masks]
    left_refs, right_refs = refs[: counts[0]], refs[counts[0] : sum(counts)]
    out_ref, low_ref, high_ref, left_s, right_s = refs[sum(counts) :]

    def normed(block_refs, block_masks, axis, held):
        where = [(ref, n, m) for ref, group in zip(block_refs, block_masks) for n, m in enumerate(group)]
        squares = None
        for ref, n, _ in where:
            values = ref[n].astype(jnp.float32)
            part = jnp.sum(values * values, axis=-1, keepdims=True)
            squares = part if squares is None else squares + part
        scale = lax.rsqrt(squares + epsilon)
        index = 0 if axis is None else lax.axis_index(axis)
        for ref, n, m in where:
            held[index ^ m] = (ref[n].astype(jnp.float32) * scale).astype(jnp.bfloat16)
        return jnp.concatenate([held[n] for n in range(len(where))], axis=1)

    left = normed(left_refs, masks[0], axes[0], left_s)
    right = normed(right_refs, masks[1], axes[1], right_s)
    volume = lax.dot_general(
        left, right, (((1,), (1,)), ((), ())), preferred_element_type=jnp.float32
    )
    blocks = LANES // tgt_cols
    inner = src_cols // blocks
    rows_a = out_ref.shape[0]
    for i in range(rows_a):
        for k in range(out_ref.shape[1]):
            pieces = [
                volume[
                    i * src_cols + b * inner : i * src_cols + (b + 1) * inner,
                    k * tgt_cols : (k + 1) * tgt_cols,
                ]
                for b in range(blocks)
            ]
            plane = jnp.concatenate(pieces, axis=1).astype(jnp.bfloat16)
            out_ref[i, k] = plane
            if i < HALO:
                low_ref[i, k] = plane
            if i >= rows_a - HALO:
                high_ref[i - rows_a + HALO, k] = plane


def weights_kernel(
    b1_ref, b2_ref, b3_ref, one_ref, two_ref, three_ref, bias_ref, w1_ref, w2_ref, w3_ref, w3_s,
    *, inner, rows_a, rows_b,
):
    channels = one_ref.shape[2]
    per_row = LANES // channels
    lane = lax.broadcasted_iota(jnp.int32, (channels, LANES), 1)
    row = lax.broadcasted_iota(jnp.int32, (channels, LANES), 0)
    lane_block = lane // channels
    spread = (lane % channels == row).astype(jnp.bfloat16)

    def tiled(values):
        return jnp.dot(values, spread, preferred_element_type=jnp.float32)

    for n, ref in enumerate((b1_ref, b2_ref, b3_ref)):
        plane = jnp.zeros((channels, LANES), jnp.float32)
        for c in range(channels):
            plane = jnp.where(row == c, ref[c if n < 2 else 0], plane)
        bias_ref[n] = plane

    def tap(a, b, e, g):
        return ((a * TAPS + b) * TAPS + e) * TAPS + g

    one = [tiled(one_ref[:, g, :]) for g in range(TAPS)]
    column = jnp.where(row < inner, row, jnp.where(row == inner, inner, -2))
    column = jnp.where(row == 2 * inner - 1, -1, column)
    slabs = []
    for a in range(TAPS):
        for e in range(TAPS):
            for g in range(TAPS):
                slab = jnp.zeros((channels, LANES), jnp.float32)
                for b in range(TAPS):
                    n = tap(a, b, e, 0) // TAPS
                    hit = (column - lane_block == b - 1) & (column >= -1)
                    slab = jnp.where(hit, one[g][n : n + 1], slab)
                slabs.append(slab)
    while (len(slabs) * channels) % LANES:
        slabs.append(jnp.zeros((channels, LANES), jnp.float32))
    w1_ref[...] = jnp.concatenate(slabs, axis=0).T.astype(jnp.bfloat16)

    two = tiled(two_ref[...])
    for b in range(TAPS):
        for half in range(2):
            col = (b * 2 + half) * LANES
            for g in range(TAPS):
                for oi in range(2):
                    for ok in range(2):
                        block = jnp.zeros((channels, LANES), jnp.float32)
                        for low in range(2):
                            a = half * 2 + low - oi
                            if not 0 <= a < TAPS:
                                continue
                            for e in range(TAPS):
                                n = tap(a, b, e, g) * channels
                                hit = lane_block == low * 4 + ok + e
                                block = jnp.where(hit, two[n : n + channels], block)
                        at = ((g * 2 + oi) * 2 + ok) * channels
                        w2_ref[at : at + channels, col : col + LANES] = block.astype(jnp.bfloat16)

    three = [tiled(three_ref[:, g, :]) for g in range(TAPS)]
    w3_s[...] = jnp.zeros_like(w3_s)
    lane_k = lax.broadcasted_iota(jnp.int32, (rows_b, LANES), 1) // channels
    row_k = lax.broadcasted_iota(jnp.int32, (rows_b, LANES), 0)
    for a in range(TAPS):
        for b in range(TAPS):
            for g in range(TAPS):
                block = jnp.zeros((rows_b, LANES), jnp.float32)
                for e in range(TAPS):
                    n = tap(a, b, e, 0) // TAPS
                    block = jnp.where(lane_k - row_k == e, three[g][n : n + 1], block)
                for oi in range(rows_a):
                    col = (oi + a) * LANES
                    at = ((g * TAPS + b) * rows_a + oi) * rows_b
                    w3_s[at : at + rows_b, col : col + LANES] = block
    w3_ref[...] = w3_s[...].astype(jnp.bfloat16)


def layers_kernel(
    bias_ref, own_ref, low_a_ref, high_a_ref, low_b_ref, high_b_ref,
    w1_ref, w2_ref, w3_ref, out_ref, vj, a1, a2, *, sizes, tgt_cols, inner, channels,
):
    rows_a, rows_b = own_ref.shape[0], own_ref.shape[1]
    ext_a, ext_b = rows_a + 2 * HALO, rows_b + 2 * HALO
    count_a, count_b = sizes[0] * rows_a, sizes[1] * rows_b
    first_a = lax.axis_index("src") * rows_a
    first_b = lax.axis_index("tgt") * rows_b

    def plane(a, b):
        if b < HALO:
            return low_b_ref[a, b]
        if b >= HALO + rows_b:
            return high_b_ref[a, b - HALO - rows_b]
        if a < HALO:
            return low_a_ref[a, b - HALO]
        if a >= HALO + rows_a:
            return high_a_ref[a - HALO - rows_a, b - HALO]
        return own_ref[a - HALO, b - HALO]

    def inside(a, b, edge):
        ga = first_a + a - edge
        gb = first_b + b - edge
        return (ga >= 0) & (ga < count_a) & (gb >= 0) & (gb < count_b)

    def lanes(rows):
        return lax.broadcasted_iota(jnp.int32, (rows, LANES), 1)

    def up(x, step, size):
        pos = lanes(x.shape[0]) % size
        return jnp.where(pos >= step, pltpu.roll(x, step, 1), 0.0)

    def down(x, step, size):
        pos = lanes(x.shape[0]) % size
        return jnp.where(pos < size - step, pltpu.roll(x, LANES - step, 1), 0.0)

    plane_row = lax.broadcasted_iota(jnp.int32, (inner, LANES), 0)

    def spread_row(a):
        for b in range(ext_b):
            x = plane(a, b).astype(jnp.float32)
            x = jnp.where(inside(a, b, HALO), x, 0.0)
            before = up(x, tgt_cols, LANES)
            after = down(x, tgt_cols, LANES)
            edge = jnp.where(plane_row == inner - 1, before, jnp.where(plane_row == 0, after, 0.0))
            both = jnp.concatenate([x, edge], axis=0)
            rows = 2 * inner
            vj[a, b, 0:rows] = up(both, 1, tgt_cols).astype(jnp.bfloat16)
            vj[a, b, rows : 2 * rows] = both.astype(jnp.bfloat16)
            vj[a, b, 2 * rows : 3 * rows] = down(both, 1, tgt_cols).astype(jnp.bfloat16)

    for a in range(ext_a):
        spread_row(a)

    def put(dst, a, b, blocks):
        dst[a, b, 0:channels] = up(blocks[-1], tgt_cols, LANES).astype(jnp.bfloat16)
        for n, block in enumerate(blocks):
            dst[a, b, (n + 1) * channels : (n + 2) * channels] = block.astype(jnp.bfloat16)
        dst[a, b, (inner + 1) * channels :] = down(blocks[0], tgt_cols, LANES).astype(jnp.bfloat16)

    l1_a, l1_b = ext_a - 2, ext_b - 2
    bias1 = bias_ref[0]
    depth1 = TAPS * TAPS * TAPS * 2 * inner
    group = 4 if l1_b % 4 == 0 else 2

    def first_row(a):
        for b0 in range(0, l1_b, group):
            x = jnp.concatenate(
                [
                    jnp.concatenate(
                        [vj[a + da, b0 + n + db] for da in range(TAPS) for db in range(TAPS)], axis=0
                    )
                    for n in range(group)
                ],
                axis=1,
            )
            got = jnp.dot(w1_ref[:, :depth1], x, preferred_element_type=jnp.float32)
            for n in range(group):
                ok = inside(a, b0 + n, HALO - 1)
                blocks = [
                    jnp.where(
                        ok,
                        jnp.maximum(
                            got[c * channels : (c + 1) * channels, n * LANES : (n + 1) * LANES]
                            + bias1,
                            0.0,
                        ),
                        0.0,
                    )
                    for c in range(inner)
                ]
                put(a1, a, b0 + n, blocks)

    for a in range(l1_a):
        first_row(a)

    l2_a, l2_b = l1_a - 2, l1_b - 2
    bias2 = bias_ref[1]
    cells = 4 * channels
    half = inner // 2

    def second_patch(pa, pb):
        for h in range(2):
            x = jnp.concatenate(
                [
                    jnp.concatenate(
                        [
                            a1[pa + wi, pb + wk, (c + dj) * channels : (c + dj + 1) * channels]
                            for dj in range(TAPS)
                            for wi in range(4)
                            for wk in range(4)
                        ],
                        axis=0,
                    )
                    for c in range(h * half, (h + 1) * half)
                ],
                axis=1,
            )
            got = jnp.dot(w2_ref[...], x, preferred_element_type=jnp.float32)
            for q in range(half):
                part = got[:, q * LANES : (q + 1) * LANES]
                total = (
                    part[cells : 2 * cells]
                    + up(part[:cells], 1, tgt_cols)
                    + down(part[2 * cells :], 1, tgt_cols)
                )
                c = h * half + q
                for oi in range(2):
                    for ok in range(2):
                        at = (oi * 2 + ok) * channels
                        block = jnp.maximum(total[at : at + channels] + bias2, 0.0)
                        block = jnp.where(inside(pa + oi, pb + ok, HALO - 2), block, 0.0)
                        a2[pa + oi, pb + ok, c * channels : (c + 1) * channels] = block.astype(
                            jnp.bfloat16
                        )

    for pa in range(0, l2_a, 2):
        for pb in range(0, l2_b, 2):
            second_patch(pa, pb)

    cells = rows_a * rows_b
    nothing = jnp.zeros((channels, LANES), jnp.bfloat16)
    parts = []
    for h in range(2):
        x = jnp.concatenate(
            [
                jnp.concatenate(
                    [
                        a2[wi, wk, c * channels : (c + 1) * channels] if wk < l2_b else nothing
                        for wi in range(l2_a)
                        for wk in range(LANES // channels)
                    ],
                    axis=0,
                )
                for c in range(h * half, (h + 1) * half)
            ],
            axis=1,
        )
        got = jnp.dot(w3_ref[...], x, preferred_element_type=jnp.float32)
        parts += [got[:, q * LANES : (q + 1) * LANES] for q in range(half)]

    def column_sum(c, g):
        total = None
        for b in range(TAPS):
            at = (g * TAPS + b) * cells
            n = c + b - 1
            if n < 0:
                part = up(parts[-1][at : at + cells], tgt_cols, LANES)
            elif n >= inner:
                part = down(parts[0][at : at + cells], tgt_cols, LANES)
            else:
                part = parts[n][at : at + cells]
            total = part if total is None else total + part
        return total

    bias3 = bias_ref[2]
    columns = [
        jnp.maximum(
            column_sum(c, 1)
            + up(column_sum(c, 0), 1, tgt_cols)
            + down(column_sum(c, 2), 1, tgt_cols)
            + bias3,
            0.0,
        )
        for c in range(inner)
    ]
    scores = jnp.stack(columns, axis=0).swapaxes(0, 1)
    for n in range(cells):
        for b in range(LANES // tgt_cols):
            out_ref[n // rows_b, n % rows_b, b * inner : (b + 1) * inner] = scores[
                n, :, b * tgt_cols : (b + 1) * tgt_cols
            ].astype(jnp.bfloat16)


VMEM = pl.BlockSpec(memory_space=pltpu.VMEM)
SMEM = pl.BlockSpec(memory_space=pltpu.SMEM)


def one_pair(source, target, conv_one, bias_one, conv_two, bias_two, conv_three, bias_three):
    rows_a, src_cols, _ = source.shape
    rows_b, tgt_cols, _ = target.shape
    channels = conv_two.shape[-1]
    blocks = LANES // tgt_cols
    inner = src_cols // blocks
    assert 2 * inner == channels and LANES % tgt_cols == 0
    assert rows_a % 2 == 0 and rows_b % 2 == 0 and min(rows_a, rows_b) >= HALO

    left, left_masks = xor_blocks(source.reshape(rows_a * src_cols, -1), "tgt")
    right, right_masks = xor_blocks(target.reshape(rows_b * tgt_cols, -1), "src")
    left, left_masks, left_axis = wide_blocks(left, left_masks, "tgt")
    right, right_masks, right_axis = wide_blocks(right, right_masks, "src")

    taps = TAPS**4
    w3_cols = (rows_a + 2) * LANES
    w3_rows = TAPS * TAPS * rows_a * rows_b
    w1_cols = -(-(TAPS**3 * channels) // LANES) * LANES
    biases, w1, w2, w3 = pl.pallas_call(
        partial(weights_kernel, inner=inner, rows_a=rows_a, rows_b=rows_b),
        out_shape=(
            jax.ShapeDtypeStruct((TAPS, channels, LANES), jnp.float32),
            jax.ShapeDtypeStruct((LANES, w1_cols), jnp.bfloat16),
            jax.ShapeDtypeStruct((TAPS * 4 * channels, TAPS * 2 * LANES), jnp.bfloat16),
            jax.ShapeDtypeStruct((w3_rows, w3_cols), jnp.bfloat16),
        ),
        in_specs=[SMEM] * 3 + [VMEM] * 3,
        out_specs=(VMEM,) * 4,
        scratch_shapes=[pltpu.VMEM((w3_rows, w3_cols), jnp.float32)],
        cost_estimate=pl.CostEstimate(flops=2_000_000_000, bytes_accessed=1_000_000, transcendentals=0),
        compiler_params=pltpu.CompilerParams(vmem_limit_bytes=8 << 20),
        name="weights",
    )(
        bias_one,
        bias_two,
        bias_three,
        conv_one.reshape(-1, TAPS, channels),
        conv_two.reshape(taps, channels, channels).swapaxes(1, 2).reshape(taps * channels, channels),
        conv_three.reshape(-1, TAPS, channels),
    )

    def held(pieces):
        return pltpu.VMEM((sum(p.shape[0] for p in pieces), *pieces[0].shape[1:]), jnp.bfloat16)

    edge = jax.ShapeDtypeStruct((HALO, rows_b, inner, LANES), jnp.bfloat16)
    own, low_edge, high_edge = pl.pallas_call(
        partial(
            volume_kernel,
            masks=(left_masks, right_masks),
            axes=(left_axis, right_axis),
            src_cols=src_cols,
            tgt_cols=tgt_cols,
        ),
        out_shape=(jax.ShapeDtypeStruct((rows_a, rows_b, inner, LANES), jnp.bfloat16), edge, edge),
        in_specs=[VMEM] * (len(left) + len(right)),
        out_specs=(VMEM,) * 3,
        scratch_shapes=[held(left), held(right)],
        compiler_params=pltpu.CompilerParams(vmem_limit_bytes=8 << 20),
        name="volume",
    )(*left, *right)

    low_a, high_a = swap_edges(low_edge, high_edge, "src")
    tall = [low_a, own, high_a]
    low_edge = jnp.concatenate([x[:, :HALO] for x in tall], axis=0)
    high_edge = jnp.concatenate([x[:, rows_b - HALO :] for x in tall], axis=0)
    low_b, high_b = swap_edges(low_edge, high_edge, "tgt")
    ext_a, ext_b = rows_a + 2 * HALO, rows_b + 2 * HALO
    return pl.pallas_call(
        partial(
            layers_kernel,
            sizes=(lax.axis_size("src"), lax.axis_size("tgt")),
            tgt_cols=tgt_cols,
            inner=inner,
            channels=channels,
        ),
        out_shape=jax.ShapeDtypeStruct((rows_a, rows_b, src_cols, tgt_cols), jnp.bfloat16),
        in_specs=[VMEM] * 9,
        out_specs=VMEM,
        scratch_shapes=[
            pltpu.VMEM((ext_a, ext_b, TAPS * 2 * inner, LANES), jnp.bfloat16),
            pltpu.VMEM((ext_a - 2, ext_b - 2, (inner + 2) * channels, LANES), jnp.bfloat16),
            pltpu.VMEM((ext_a - 4, ext_b - 4, inner * channels, LANES), jnp.bfloat16),
        ],
        compiler_params=pltpu.CompilerParams(vmem_limit_bytes=20 << 20),
        name="layers",
    )(biases, own, low_a, high_a, low_b, high_b, w1, w2, w3)


def local(source_feats, target_feats, *params):
    return jnp.stack(
        [one_pair(source_feats[p], target_feats[p], *params) for p in range(source_feats.shape[0])]
    )


def solution(mesh):
    return jax.shard_map(
        local,
        mesh=mesh,
        in_specs=(
            P(None, "src", None, "tgt"),
            P(None, "tgt", None, "src"),
            P(),
            P(),
            P(),
            P(),
            P(),
            P(),
        ),
        out_specs=P(None, "src", "tgt", None, None),
        check_vma=False,
    )
```

```python
from functools import partial

import jax
import jax.numpy as jnp
from jax import lax
from jax.experimental import pallas as pl
from jax.experimental.pallas import tpu as pltpu
from jax.sharding import PartitionSpec as P

LANES = 128
TAPS = 3
HALO = 3
epsilon = 1e-06


def copy_kernel(in_ref, out_ref):
    out_ref[...] = in_ref[...]


def on_chip(block):
    return pl.pallas_call(
        copy_kernel,
        out_shape=jax.ShapeDtypeStruct(block.shape, block.dtype),
        in_specs=[pl.BlockSpec(memory_space=pltpu.VMEM)],
        out_specs=pl.BlockSpec(memory_space=pltpu.VMEM),
        cost_estimate=pl.CostEstimate(flops=1_000_000_000, bytes_accessed=0, transcendentals=0),
        compiler_params=pltpu.CompilerParams(vmem_limit_bytes=4 << 20),
        name="own",
    )(block)


def xor_blocks(block, axis):
    count = lax.axis_size(axis)
    held, masks = block[None], [0]
    pieces, piece_masks = [held], [[0]]
    step = count // 2
    while step:
        swap = [(i, i ^ step) for i in range(count)]
        got = lax.ppermute(held, axis, swap)
        if len(masks) == 1:
            held = on_chip(held)
        got_masks = [m ^ step for m in masks]
        pieces.append(got)
        piece_masks.append(got_masks)
        masks = masks + got_masks
        if step > 1:
            held = jnp.concatenate([held, got], axis=0)
        step //= 2
    return pieces, piece_masks


def swap_edges(low_edge, high_edge, axis):
    count = lax.axis_size(axis)
    forward = [(i, (i + 1) % count) for i in range(count)]
    backward = [((i + 1) % count, i) for i in range(count)]
    return lax.ppermute(high_edge, axis, forward), lax.ppermute(low_edge, axis, backward)


def wide_blocks(pieces, masks, axis):
    chunk = pieces[0].shape[-1]
    if chunk % LANES == 0:
        return pieces, masks, axis
    flat = [m for group in masks for m in group]
    blocks = jnp.concatenate(pieces, axis=0)
    place = [flat.index(m) for m in range(len(flat))]
    order = jnp.asarray(place, jnp.int32)[lax.axis_index(axis) ^ jnp.arange(len(flat))]
    joined = jnp.take(blocks, order, axis=0).transpose(1, 0, 2)
    return [joined.reshape(1, joined.shape[0], -1)], [[0]], None


def volume_kernel(*refs, masks, axes, src_cols, tgt_cols):
    counts = [len(group) for group in masks]
    left_refs, right_refs = refs[: counts[0]], refs[counts[0] : sum(counts)]
    out_ref, low_ref, high_ref, left_s, right_s = refs[sum(counts) :]

    def normed(block_refs, block_masks, axis, held):
        where = [(ref, n, m) for ref, group in zip(block_refs, block_masks) for n, m in enumerate(group)]
        squares = None
        for ref, n, _ in where:
            values = ref[n].astype(jnp.float32)
            part = jnp.sum(values * values, axis=-1, keepdims=True)
            squares = part if squares is None else squares + part
        scale = lax.rsqrt(squares + epsilon)
        index = 0 if axis is None else lax.axis_index(axis)
        for ref, n, m in where:
            held[index ^ m] = (ref[n].astype(jnp.float32) * scale).astype(jnp.bfloat16)
        return jnp.concatenate([held[n] for n in range(len(where))], axis=1)

    left = normed(left_refs, masks[0], axes[0], left_s)
    right = normed(right_refs, masks[1], axes[1], right_s)
    volume = lax.dot_general(
        left, right, (((1,), (1,)), ((), ())), preferred_element_type=jnp.float32
    )
    blocks = LANES // tgt_cols
    inner = src_cols // blocks
    rows_a = out_ref.shape[0]
    for i in range(rows_a):
        for k in range(out_ref.shape[1]):
            pieces = [
                volume[
                    i * src_cols + b * inner : i * src_cols + (b + 1) * inner,
                    k * tgt_cols : (k + 1) * tgt_cols,
                ]
                for b in range(blocks)
            ]
            plane = jnp.concatenate(pieces, axis=1).astype(jnp.bfloat16)
            out_ref[i, k] = plane
            if i < HALO:
                low_ref[i, k] = plane
            if i >= rows_a - HALO:
                high_ref[i - rows_a + HALO, k] = plane


def first_tiles():
    tiles = [(0, ((a, e, 0), (a, e, 1))) for a in range(TAPS) for e in range(TAPS)]
    tiles += [(1, ((a, 0, 2), (a, 1, 2))) for a in range(TAPS)]
    tiles += [(2, ((0, 2, 2), (1, 2, 2))), (1, ((2, 2, 2), None))]
    return tiles


def weights_kernel(
    b1_ref, b2_ref, b3_ref, one_ref, two_ref, three_ref, bias_ref, w1_ref, w2_ref, w3_ref, w3_s,
    *, inner, rows_a, rows_b,
):
    channels = one_ref.shape[2]
    per_row = LANES // channels
    lane = lax.broadcasted_iota(jnp.int32, (channels, LANES), 1)
    row = lax.broadcasted_iota(jnp.int32, (channels, LANES), 0)
    lane_block = lane // channels
    spread = (lane % channels == row).astype(jnp.bfloat16)

    def tiled(values):
        return jnp.dot(values, spread, preferred_element_type=jnp.float32)

    for n, ref in enumerate((b1_ref, b2_ref, b3_ref)):
        plane = jnp.zeros((channels, LANES), jnp.float32)
        for c in range(channels):
            plane = jnp.where(row == c, ref[c if n < 2 else 0], plane)
        bias_ref[n] = plane

    def tap(a, b, e, g):
        return ((a * TAPS + b) * TAPS + e) * TAPS + g

    one = [tiled(one_ref[:, g, :]) for g in range(TAPS)]
    column = lax.broadcasted_iota(jnp.int32, (inner, LANES), 0)
    half_block = lax.broadcasted_iota(jnp.int32, (inner, LANES), 1) // channels

    def half_slab(part):
        main = jnp.zeros((inner, LANES), jnp.float32)
        side = jnp.zeros((inner, LANES), jnp.float32)
        if part is not None:
            a, e, g = part
            for b in range(TAPS):
                n = tap(a, b, e, 0) // TAPS
                value = one[g][n : n + 1]
                main = jnp.where(column - half_block == b - 1, value, main)
                if b == 0:
                    side = jnp.where((column == inner - 1) & (half_block == 0), value, side)
                if b == TAPS - 1:
                    side = jnp.where((column == 0) & (half_block == 1), value, side)
        return jnp.concatenate([main, side], axis=1)

    slabs = [half_slab(part) for _, parts in first_tiles() for part in parts]
    while (len(slabs) * inner) % LANES:
        slabs.append(jnp.zeros((inner, 2 * LANES), jnp.float32))
    w1_ref[...] = jnp.concatenate(slabs, axis=0).T.astype(jnp.bfloat16)

    two = tiled(two_ref[...])
    for b in range(TAPS):
        for half in range(2):
            col = (b * 2 + half) * LANES
            for g in range(TAPS):
                for oi in range(2):
                    for ok in range(2):
                        block = jnp.zeros((channels, LANES), jnp.float32)
                        for low in range(2):
                            a = half * 2 + low - oi
                            if not 0 <= a < TAPS:
                                continue
                            for e in range(TAPS):
                                n = tap(a, b, e, g) * channels
                                hit = lane_block == low * 4 + ok + e
                                block = jnp.where(hit, two[n : n + channels], block)
                        at = ((g * 2 + oi) * 2 + ok) * channels
                        w2_ref[at : at + channels, col : col + LANES] = block.astype(jnp.bfloat16)

    three = [tiled(three_ref[:, g, :]) for g in range(TAPS)]
    w3_s[...] = jnp.zeros_like(w3_s)
    lane_k = lax.broadcasted_iota(jnp.int32, (rows_b, LANES), 1) // channels
    row_k = lax.broadcasted_iota(jnp.int32, (rows_b, LANES), 0)
    for a in range(TAPS):
        for b in range(TAPS):
            for g in range(TAPS):
                block = jnp.zeros((rows_b, LANES), jnp.float32)
                for e in range(TAPS):
                    n = tap(a, b, e, 0) // TAPS
                    block = jnp.where(lane_k - row_k == e, three[g][n : n + 1], block)
                for oi in range(rows_a):
                    col = (oi + a) * LANES
                    at = ((g * TAPS + b) * rows_a + oi) * rows_b
                    w3_s[at : at + rows_b, col : col + LANES] = block
    w3_ref[...] = w3_s[...].astype(jnp.bfloat16)


def layers_kernel(
    bias_ref, own_ref, low_a_ref, high_a_ref, low_b_ref, high_b_ref,
    w1_ref, w2_ref, w3_ref, out_ref, vj, a1, a2, *, sizes, tgt_cols, inner, channels,
):
    rows_a, rows_b = own_ref.shape[0], own_ref.shape[1]
    ext_a, ext_b = rows_a + 2 * HALO, rows_b + 2 * HALO
    count_a, count_b = sizes[0] * rows_a, sizes[1] * rows_b
    first_a = lax.axis_index("src") * rows_a
    first_b = lax.axis_index("tgt") * rows_b

    def plane(a, b):
        if b < HALO:
            return low_b_ref[a, b]
        if b >= HALO + rows_b:
            return high_b_ref[a, b - HALO - rows_b]
        if a < HALO:
            return low_a_ref[a, b - HALO]
        if a >= HALO + rows_a:
            return high_a_ref[a - HALO - rows_a, b - HALO]
        return own_ref[a - HALO, b - HALO]

    def inside(a, b, edge):
        ga = first_a + a - edge
        gb = first_b + b - edge
        return (ga >= 0) & (ga < count_a) & (gb >= 0) & (gb < count_b)

    def lanes(rows):
        return lax.broadcasted_iota(jnp.int32, (rows, LANES), 1)

    def up(x, step, size):
        pos = lanes(x.shape[0]) % size
        return jnp.where(pos >= step, pltpu.roll(x, step, 1), 0.0)

    def down(x, step, size):
        pos = lanes(x.shape[0]) % size
        return jnp.where(pos < size - step, pltpu.roll(x, LANES - step, 1), 0.0)

    above = None
    for a in range(ext_a):
        shifted = []
        for b in range(ext_b):
            x = jnp.where(inside(a, b, HALO), plane(a, b).astype(jnp.float32), 0.0)
            vj[0, a, b] = jnp.concatenate([up(x, 1, tgt_cols), x], axis=0).astype(jnp.bfloat16)
            shifted.append(down(x, 1, tgt_cols))
        for b in range(ext_b):
            beside = shifted[b + 1] if b + 1 < ext_b else jnp.zeros_like(shifted[b])
            vj[1, a, b] = jnp.concatenate([shifted[b], beside], axis=0).astype(jnp.bfloat16)
            if above is not None:
                vj[2, a - 1, b] = jnp.concatenate([above[b], shifted[b]], axis=0).astype(jnp.bfloat16)
        above = shifted

    def put(dst, a, b, blocks):
        dst[a, b, 0:channels] = up(blocks[-1], tgt_cols, LANES).astype(jnp.bfloat16)
        for n, block in enumerate(blocks):
            dst[a, b, (n + 1) * channels : (n + 2) * channels] = block.astype(jnp.bfloat16)
        dst[a, b, (inner + 1) * channels :] = down(blocks[0], tgt_cols, LANES).astype(jnp.bfloat16)

    l1_a, l1_b = ext_a - 2, ext_b - 2
    bias1 = bias_ref[0]
    depth1 = len(first_tiles()) * 2 * inner
    rows1 = (inner + 2) * channels
    group = 4 if l1_b % 4 == 0 else 2

    def first_row(a):
        for b0 in range(0, l1_b, group):
            x = jnp.concatenate(
                [
                    jnp.concatenate(
                        [
                            vj[kind, a + parts[0][0], b0 + n + parts[0][1]]
                            for kind, parts in first_tiles()
                        ],
                        axis=0,
                    )
                    for n in range(group)
                ],
                axis=1,
            )
            got = jnp.dot(w1_ref[:rows1, :depth1], x, preferred_element_type=jnp.float32)
            for n in range(group):
                ok = inside(a, b0 + n, HALO - 1)
                part = got[:, n * LANES : (n + 1) * LANES]
                sums = [part[c * channels : (c + 1) * channels] for c in range(inner + 2)]
                sums[0] = sums[0] + up(sums[inner], tgt_cols, LANES)
                sums[inner - 1] = sums[inner - 1] + down(sums[inner + 1], tgt_cols, LANES)
                blocks = [jnp.where(ok, jnp.maximum(x + bias1, 0.0), 0.0) for x in sums[:inner]]
                put(a1, a, b0 + n, blocks)

    for a in range(l1_a):
        first_row(a)

    l2_a, l2_b = l1_a - 2, l1_b - 2
    bias2 = bias_ref[1]
    cells = 4 * channels
    half = inner // 2

    def second_patch(pa, pb):
        for h in range(2):
            x = jnp.concatenate(
                [
                    jnp.concatenate(
                        [
                            a1[pa + wi, pb + wk, (c + dj) * channels : (c + dj + 1) * channels]
                            for dj in range(TAPS)
                            for wi in range(4)
                            for wk in range(4)
                        ],
                        axis=0,
                    )
                    for c in range(h * half, (h + 1) * half)
                ],
                axis=1,
            )
            got = jnp.dot(w2_ref[...], x, preferred_element_type=jnp.float32)
            for q in range(half):
                part = got[:, q * LANES : (q + 1) * LANES]
                total = (
                    part[cells : 2 * cells]
                    + up(part[:cells], 1, tgt_cols)
                    + down(part[2 * cells :], 1, tgt_cols)
                )
                c = h * half + q
                for oi in range(2):
                    for ok in range(2):
                        at = (oi * 2 + ok) * channels
                        block = jnp.maximum(total[at : at + channels] + bias2, 0.0)
                        block = jnp.where(inside(pa + oi, pb + ok, HALO - 2), block, 0.0)
                        a2[pa + oi, pb + ok, c * channels : (c + 1) * channels] = block.astype(
                            jnp.bfloat16
                        )

    for pa in range(0, l2_a, 2):
        for pb in range(0, l2_b, 2):
            second_patch(pa, pb)

    cells = rows_a * rows_b
    nothing = jnp.zeros((channels, LANES), jnp.bfloat16)
    parts = []
    for h in range(2):
        x = jnp.concatenate(
            [
                jnp.concatenate(
                    [
                        a2[wi, wk, c * channels : (c + 1) * channels] if wk < l2_b else nothing
                        for wi in range(l2_a)
                        for wk in range(LANES // channels)
                    ],
                    axis=0,
                )
                for c in range(h * half, (h + 1) * half)
            ],
            axis=1,
        )
        got = jnp.dot(w3_ref[...], x, preferred_element_type=jnp.float32)
        parts += [got[:, q * LANES : (q + 1) * LANES] for q in range(half)]

    def column_sum(c, g):
        total = None
        for b in range(TAPS):
            at = (g * TAPS + b) * cells
            n = c + b - 1
            if n < 0:
                part = up(parts[-1][at : at + cells], tgt_cols, LANES)
            elif n >= inner:
                part = down(parts[0][at : at + cells], tgt_cols, LANES)
            else:
                part = parts[n][at : at + cells]
            total = part if total is None else total + part
        return total

    bias3 = bias_ref[2]
    columns = [
        jnp.maximum(
            column_sum(c, 1)
            + up(column_sum(c, 0), 1, tgt_cols)
            + down(column_sum(c, 2), 1, tgt_cols)
            + bias3,
            0.0,
        )
        for c in range(inner)
    ]
    scores = jnp.stack(columns, axis=0).swapaxes(0, 1)
    for n in range(cells):
        for b in range(LANES // tgt_cols):
            out_ref[n // rows_b, n % rows_b, b * inner : (b + 1) * inner] = scores[
                n, :, b * tgt_cols : (b + 1) * tgt_cols
            ].astype(jnp.bfloat16)


VMEM = pl.BlockSpec(memory_space=pltpu.VMEM)
SMEM = pl.BlockSpec(memory_space=pltpu.SMEM)


def one_pair(source, target, conv_one, bias_one, conv_two, bias_two, conv_three, bias_three):
    rows_a, src_cols, _ = source.shape
    rows_b, tgt_cols, _ = target.shape
    channels = conv_two.shape[-1]
    blocks = LANES // tgt_cols
    inner = src_cols // blocks
    assert 2 * inner == channels and LANES % tgt_cols == 0
    assert rows_a % 2 == 0 and rows_b % 2 == 0 and min(rows_a, rows_b) >= HALO

    left, left_masks = xor_blocks(source.reshape(rows_a * src_cols, -1), "tgt")
    right, right_masks = xor_blocks(target.reshape(rows_b * tgt_cols, -1), "src")
    left, left_masks, left_axis = wide_blocks(left, left_masks, "tgt")
    right, right_masks, right_axis = wide_blocks(right, right_masks, "src")

    taps = TAPS**4
    w3_cols = (rows_a + 2) * LANES
    w3_rows = TAPS * TAPS * rows_a * rows_b
    w1_cols = -(-(len(first_tiles()) * 2 * inner) // LANES) * LANES
    biases, w1, w2, w3 = pl.pallas_call(
        partial(weights_kernel, inner=inner, rows_a=rows_a, rows_b=rows_b),
        out_shape=(
            jax.ShapeDtypeStruct((TAPS, channels, LANES), jnp.float32),
            jax.ShapeDtypeStruct((2 * LANES, w1_cols), jnp.bfloat16),
            jax.ShapeDtypeStruct((TAPS * 4 * channels, TAPS * 2 * LANES), jnp.bfloat16),
            jax.ShapeDtypeStruct((w3_rows, w3_cols), jnp.bfloat16),
        ),
        in_specs=[SMEM] * 3 + [VMEM] * 3,
        out_specs=(VMEM,) * 4,
        scratch_shapes=[pltpu.VMEM((w3_rows, w3_cols), jnp.float32)],
        cost_estimate=pl.CostEstimate(flops=2_000_000_000, bytes_accessed=1_000_000, transcendentals=0),
        compiler_params=pltpu.CompilerParams(vmem_limit_bytes=8 << 20),
        name="weights",
    )(
        bias_one,
        bias_two,
        bias_three,
        conv_one.reshape(-1, TAPS, channels),
        conv_two.reshape(taps, channels, channels).swapaxes(1, 2).reshape(taps * channels, channels),
        conv_three.reshape(-1, TAPS, channels),
    )

    def held(pieces):
        return pltpu.VMEM((sum(p.shape[0] for p in pieces), *pieces[0].shape[1:]), jnp.bfloat16)

    edge = jax.ShapeDtypeStruct((HALO, rows_b, inner, LANES), jnp.bfloat16)
    own, low_edge, high_edge = pl.pallas_call(
        partial(
            volume_kernel,
            masks=(left_masks, right_masks),
            axes=(left_axis, right_axis),
            src_cols=src_cols,
            tgt_cols=tgt_cols,
        ),
        out_shape=(jax.ShapeDtypeStruct((rows_a, rows_b, inner, LANES), jnp.bfloat16), edge, edge),
        in_specs=[VMEM] * (len(left) + len(right)),
        out_specs=(VMEM,) * 3,
        scratch_shapes=[held(left), held(right)],
        compiler_params=pltpu.CompilerParams(vmem_limit_bytes=8 << 20),
        name="volume",
    )(*left, *right)

    low_a, high_a = swap_edges(low_edge, high_edge, "src")
    tall = [low_a, own, high_a]
    low_edge = jnp.concatenate([x[:, :HALO] for x in tall], axis=0)
    high_edge = jnp.concatenate([x[:, rows_b - HALO :] for x in tall], axis=0)
    low_b, high_b = swap_edges(low_edge, high_edge, "tgt")
    ext_a, ext_b = rows_a + 2 * HALO, rows_b + 2 * HALO
    return pl.pallas_call(
        partial(
            layers_kernel,
            sizes=(lax.axis_size("src"), lax.axis_size("tgt")),
            tgt_cols=tgt_cols,
            inner=inner,
            channels=channels,
        ),
        out_shape=jax.ShapeDtypeStruct((rows_a, rows_b, src_cols, tgt_cols), jnp.bfloat16),
        in_specs=[VMEM] * 9,
        out_specs=VMEM,
        scratch_shapes=[
            pltpu.VMEM((TAPS, ext_a, ext_b, 2 * inner, LANES), jnp.bfloat16),
            pltpu.VMEM((ext_a - 2, ext_b - 2, (inner + 2) * channels, LANES), jnp.bfloat16),
            pltpu.VMEM((ext_a - 4, ext_b - 4, inner * channels, LANES), jnp.bfloat16),
        ],
        compiler_params=pltpu.CompilerParams(vmem_limit_bytes=20 << 20),
        name="layers",
    )(biases, own, low_a, high_a, low_b, high_b, w1, w2, w3)


def local(source_feats, target_feats, *params):
    return jnp.stack(
        [one_pair(source_feats[p], target_feats[p], *params) for p in range(source_feats.shape[0])]
    )


def solution(mesh):
    return jax.shard_map(
        local,
        mesh=mesh,
        in_specs=(
            P(None, "src", None, "tgt"),
            P(None, "tgt", None, "src"),
            P(),
            P(),
            P(),
            P(),
            P(),
            P(),
        ),
        out_specs=P(None, "src", "tgt", None, None),
        check_vma=False,
    )
```

```python
from functools import partial

import jax
import jax.numpy as jnp
from jax import lax
from jax.experimental import pallas as pl
from jax.experimental.pallas import tpu as pltpu
from jax.sharding import PartitionSpec as P

LANES = 128
TAPS = 3
HALO = 3
epsilon = 1e-06


def copy_kernel(in_ref, out_ref):
    out_ref[...] = in_ref[...]


def on_chip(block):
    return pl.pallas_call(
        copy_kernel,
        out_shape=jax.ShapeDtypeStruct(block.shape, block.dtype),
        in_specs=[pl.BlockSpec(memory_space=pltpu.VMEM)],
        out_specs=pl.BlockSpec(memory_space=pltpu.VMEM),
        cost_estimate=pl.CostEstimate(flops=1_000_000_000, bytes_accessed=0, transcendentals=0),
        compiler_params=pltpu.CompilerParams(vmem_limit_bytes=4 << 20),
        name="own",
    )(block)


def xor_blocks(block, axis):
    count = lax.axis_size(axis)
    held, masks = block[None], [0]
    pieces, piece_masks = [held], [[0]]
    step = count // 2
    while step:
        swap = [(i, i ^ step) for i in range(count)]
        got = lax.ppermute(held, axis, swap)
        if len(masks) == 1:
            held = on_chip(held)
            pieces[0] = held
        got_masks = [m ^ step for m in masks]
        pieces.append(got)
        piece_masks.append(got_masks)
        masks = masks + got_masks
        if step > 1:
            held = jnp.concatenate([held, got], axis=0)
        step //= 2
    return pieces, piece_masks


def swap_edges(low_edge, high_edge, axis):
    count = lax.axis_size(axis)
    forward = [(i, (i + 1) % count) for i in range(count)]
    backward = [((i + 1) % count, i) for i in range(count)]
    return lax.ppermute(high_edge, axis, forward), lax.ppermute(low_edge, axis, backward)


def wide_blocks(pieces, masks, axis):
    chunk = pieces[0].shape[-1]
    if chunk % LANES == 0:
        return pieces, masks, axis
    flat = [m for group in masks for m in group]
    blocks = jnp.concatenate(pieces, axis=0)
    place = [flat.index(m) for m in range(len(flat))]
    order = jnp.asarray(place, jnp.int32)[lax.axis_index(axis) ^ jnp.arange(len(flat))]
    joined = jnp.take(blocks, order, axis=0).transpose(1, 0, 2)
    return [joined.reshape(1, joined.shape[0], -1)], [[0]], None


def volume_kernel(*refs, masks, axes, src_cols, tgt_cols):
    counts = [len(group) for group in masks]
    left_refs, right_refs = refs[: counts[0]], refs[counts[0] : sum(counts)]
    out_ref, low_ref, high_ref, left_s, right_s = refs[sum(counts) :]

    def normed(block_refs, block_masks, axis, held):
        where = [(ref, n, m) for ref, group in zip(block_refs, block_masks) for n, m in enumerate(group)]
        squares = None
        for ref, n, _ in where:
            values = ref[n].astype(jnp.float32)
            part = jnp.sum(values * values, axis=-1, keepdims=True)
            squares = part if squares is None else squares + part
        scale = lax.rsqrt(squares + epsilon)
        index = 0 if axis is None else lax.axis_index(axis)
        for ref, n, m in where:
            held[index ^ m] = (ref[n].astype(jnp.float32) * scale).astype(jnp.bfloat16)
        return jnp.concatenate([held[n] for n in range(len(where))], axis=1)

    left = normed(left_refs, masks[0], axes[0], left_s)
    right = normed(right_refs, masks[1], axes[1], right_s)
    volume = lax.dot_general(
        left, right, (((1,), (1,)), ((), ())), preferred_element_type=jnp.float32
    )
    blocks = LANES // tgt_cols
    inner = src_cols // blocks
    rows_a = out_ref.shape[0]
    for i in range(rows_a):
        for k in range(out_ref.shape[1]):
            pieces = [
                volume[
                    i * src_cols + b * inner : i * src_cols + (b + 1) * inner,
                    k * tgt_cols : (k + 1) * tgt_cols,
                ]
                for b in range(blocks)
            ]
            plane = jnp.concatenate(pieces, axis=1).astype(jnp.bfloat16)
            out_ref[i, k] = plane
            if i < HALO:
                low_ref[i, k] = plane
            if i >= rows_a - HALO:
                high_ref[i - rows_a + HALO, k] = plane


def first_tiles():
    tiles = [(0, ((a, e, 0), (a, e, 1))) for a in range(TAPS) for e in range(TAPS)]
    tiles += [(1, ((a, 0, 2), (a, 1, 2))) for a in range(TAPS)]
    tiles += [(2, ((0, 2, 2), (1, 2, 2))), (1, ((2, 2, 2), None))]
    return tiles


def weights_kernel(
    b1_ref, b2_ref, b3_ref, one_ref, two_ref, three_ref, bias_ref, w1_ref, w2_ref, w3_ref, w3_s,
    *, inner, rows_a, rows_b,
):
    channels = one_ref.shape[2]
    per_row = LANES // channels
    lane = lax.broadcasted_iota(jnp.int32, (channels, LANES), 1)
    row = lax.broadcasted_iota(jnp.int32, (channels, LANES), 0)
    lane_block = lane // channels
    spread = (lane % channels == row).astype(jnp.bfloat16)

    def tiled(values):
        return jnp.dot(values, spread, preferred_element_type=jnp.float32)

    for n, ref in enumerate((b1_ref, b2_ref, b3_ref)):
        plane = jnp.zeros((channels, LANES), jnp.float32)
        for c in range(channels):
            plane = jnp.where(row == c, ref[c if n < 2 else 0], plane)
        bias_ref[n] = plane

    def tap(a, b, e, g):
        return ((a * TAPS + b) * TAPS + e) * TAPS + g

    one = [tiled(one_ref[:, g, :]) for g in range(TAPS)]
    column = lax.broadcasted_iota(jnp.int32, (inner, LANES), 0)
    half_block = lax.broadcasted_iota(jnp.int32, (inner, LANES), 1) // channels

    def half_slab(part):
        main = jnp.zeros((inner, LANES), jnp.float32)
        side = jnp.zeros((inner, LANES), jnp.float32)
        if part is not None:
            a, e, g = part
            for b in range(TAPS):
                n = tap(a, b, e, 0) // TAPS
                value = one[g][n : n + 1]
                main = jnp.where(column - half_block == b - 1, value, main)
                if b == 0:
                    side = jnp.where((column == inner - 1) & (half_block == 0), value, side)
                if b == TAPS - 1:
                    side = jnp.where((column == 0) & (half_block == 1), value, side)
        return jnp.concatenate([main, side], axis=1)

    slabs = [half_slab(part) for _, parts in first_tiles() for part in parts]
    while (len(slabs) * inner) % LANES:
        slabs.append(jnp.zeros((inner, 2 * LANES), jnp.float32))
    w1_ref[...] = jnp.concatenate(slabs, axis=0).T.astype(jnp.bfloat16)

    two = tiled(two_ref[...])
    for b in range(TAPS):
        for half in range(2):
            col = (b * 2 + half) * LANES
            for g in range(TAPS):
                for oi in range(2):
                    for ok in range(2):
                        block = jnp.zeros((channels, LANES), jnp.float32)
                        for low in range(2):
                            a = half * 2 + low - oi
                            if not 0 <= a < TAPS:
                                continue
                            for e in range(TAPS):
                                n = tap(a, b, e, g) * channels
                                hit = lane_block == low * 4 + ok + e
                                block = jnp.where(hit, two[n : n + channels], block)
                        at = ((g * 2 + oi) * 2 + ok) * channels
                        w2_ref[at : at + channels, col : col + LANES] = block.astype(jnp.bfloat16)

    three = [tiled(three_ref[:, g, :]) for g in range(TAPS)]
    w3_s[...] = jnp.zeros_like(w3_s)
    lane_k = lax.broadcasted_iota(jnp.int32, (rows_b, LANES), 1) // channels
    row_k = lax.broadcasted_iota(jnp.int32, (rows_b, LANES), 0)
    for a in range(TAPS):
        for b in range(TAPS):
            for g in range(TAPS):
                block = jnp.zeros((rows_b, LANES), jnp.float32)
                for e in range(TAPS):
                    n = tap(a, b, e, 0) // TAPS
                    block = jnp.where(lane_k - row_k == e, three[g][n : n + 1], block)
                for oi in range(rows_a):
                    col = (oi + a) * LANES
                    at = ((g * TAPS + b) * rows_a + oi) * rows_b
                    w3_s[at : at + rows_b, col : col + LANES] = block
    w3_ref[...] = w3_s[...].astype(jnp.bfloat16)


def layers_kernel(
    bias_ref, own_ref, low_a_ref, high_a_ref, low_b_ref, high_b_ref,
    w1_ref, w2_ref, w3_ref, out_ref, vj, a1, a2, *, sizes, tgt_cols, inner, channels,
):
    rows_a, rows_b = own_ref.shape[0], own_ref.shape[1]
    ext_a, ext_b = rows_a + 2 * HALO, rows_b + 2 * HALO
    count_a, count_b = sizes[0] * rows_a, sizes[1] * rows_b
    first_a = lax.axis_index("src") * rows_a
    first_b = lax.axis_index("tgt") * rows_b

    def plane(a, b):
        if b < HALO:
            return low_b_ref[a, b]
        if b >= HALO + rows_b:
            return high_b_ref[a, b - HALO - rows_b]
        if a < HALO:
            return low_a_ref[a, b - HALO]
        if a >= HALO + rows_a:
            return high_a_ref[a - HALO - rows_a, b - HALO]
        return own_ref[a - HALO, b - HALO]

    def inside(a, b, edge):
        ga = first_a + a - edge
        gb = first_b + b - edge
        return (ga >= 0) & (ga < count_a) & (gb >= 0) & (gb < count_b)

    def lanes(rows):
        return lax.broadcasted_iota(jnp.int32, (rows, LANES), 1)

    def up(x, step, size):
        pos = lanes(x.shape[0]) % size
        return jnp.where(pos >= step, pltpu.roll(x, step, 1), 0.0)

    def down(x, step, size):
        pos = lanes(x.shape[0]) % size
        return jnp.where(pos < size - step, pltpu.roll(x, LANES - step, 1), 0.0)

    above = None
    for a in range(ext_a):
        shifted = []
        for b in range(ext_b):
            x = jnp.where(inside(a, b, HALO), plane(a, b).astype(jnp.float32), 0.0)
            vj[0, a, b] = jnp.concatenate([up(x, 1, tgt_cols), x], axis=0).astype(jnp.bfloat16)
            shifted.append(down(x, 1, tgt_cols))
        for b in range(ext_b):
            beside = shifted[b + 1] if b + 1 < ext_b else jnp.zeros_like(shifted[b])
            vj[1, a, b] = jnp.concatenate([shifted[b], beside], axis=0).astype(jnp.bfloat16)
            if above is not None:
                vj[2, a - 1, b] = jnp.concatenate([above[b], shifted[b]], axis=0).astype(jnp.bfloat16)
        above = shifted

    def put(dst, a, b, blocks):
        dst[a, b, 0:channels] = up(blocks[-1], tgt_cols, LANES).astype(jnp.bfloat16)
        for n, block in enumerate(blocks):
            dst[a, b, (n + 1) * channels : (n + 2) * channels] = block.astype(jnp.bfloat16)
        dst[a, b, (inner + 1) * channels :] = down(blocks[0], tgt_cols, LANES).astype(jnp.bfloat16)

    l1_a, l1_b = ext_a - 2, ext_b - 2
    bias1 = bias_ref[0]
    depth1 = len(first_tiles()) * 2 * inner
    rows1 = (inner + 2) * channels
    group = 4 if l1_b % 4 == 0 else 2

    def first_row(a):
        for b0 in range(0, l1_b, group):
            x = jnp.concatenate(
                [
                    jnp.concatenate(
                        [
                            vj[kind, a + parts[0][0], b0 + n + parts[0][1]]
                            for kind, parts in first_tiles()
                        ],
                        axis=0,
                    )
                    for n in range(group)
                ],
                axis=1,
            )
            got = jnp.dot(w1_ref[:rows1, :depth1], x, preferred_element_type=jnp.float32)
            for n in range(group):
                ok = inside(a, b0 + n, HALO - 1)
                part = got[:, n * LANES : (n + 1) * LANES]
                sums = [part[c * channels : (c + 1) * channels] for c in range(inner + 2)]
                sums[0] = sums[0] + up(sums[inner], tgt_cols, LANES)
                sums[inner - 1] = sums[inner - 1] + down(sums[inner + 1], tgt_cols, LANES)
                blocks = [jnp.where(ok, jnp.maximum(x + bias1, 0.0), 0.0) for x in sums[:inner]]
                put(a1, a, b0 + n, blocks)

    for a in range(l1_a):
        first_row(a)

    l2_a, l2_b = l1_a - 2, l1_b - 2
    bias2 = bias_ref[1]
    cells = 4 * channels
    half = inner // 2

    def second_patch(pa, pb):
        for h in range(2):
            x = jnp.concatenate(
                [
                    jnp.concatenate(
                        [
                            a1[pa + wi, pb + wk, (c + dj) * channels : (c + dj + 1) * channels]
                            for dj in range(TAPS)
                            for wi in range(4)
                            for wk in range(4)
                        ],
                        axis=0,
                    )
                    for c in range(h * half, (h + 1) * half)
                ],
                axis=1,
            )
            got = jnp.dot(w2_ref[...], x, preferred_element_type=jnp.float32)
            for q in range(half):
                part = got[:, q * LANES : (q + 1) * LANES]
                total = (
                    part[cells : 2 * cells]
                    + up(part[:cells], 1, tgt_cols)
                    + down(part[2 * cells :], 1, tgt_cols)
                )
                c = h * half + q
                for oi in range(2):
                    for ok in range(2):
                        at = (oi * 2 + ok) * channels
                        block = jnp.maximum(total[at : at + channels] + bias2, 0.0)
                        block = jnp.where(inside(pa + oi, pb + ok, HALO - 2), block, 0.0)
                        a2[pa + oi, pb + ok, c * channels : (c + 1) * channels] = block.astype(
                            jnp.bfloat16
                        )

    for pa in range(0, l2_a, 2):
        for pb in range(0, l2_b, 2):
            second_patch(pa, pb)

    cells = rows_a * rows_b
    nothing = jnp.zeros((channels, LANES), jnp.bfloat16)
    parts = []
    for h in range(2):
        x = jnp.concatenate(
            [
                jnp.concatenate(
                    [
                        a2[wi, wk, c * channels : (c + 1) * channels] if wk < l2_b else nothing
                        for wi in range(l2_a)
                        for wk in range(LANES // channels)
                    ],
                    axis=0,
                )
                for c in range(h * half, (h + 1) * half)
            ],
            axis=1,
        )
        got = jnp.dot(w3_ref[...], x, preferred_element_type=jnp.float32)
        parts += [got[:, q * LANES : (q + 1) * LANES] for q in range(half)]

    def column_sum(c, g):
        total = None
        for b in range(TAPS):
            at = (g * TAPS + b) * cells
            n = c + b - 1
            if n < 0:
                part = up(parts[-1][at : at + cells], tgt_cols, LANES)
            elif n >= inner:
                part = down(parts[0][at : at + cells], tgt_cols, LANES)
            else:
                part = parts[n][at : at + cells]
            total = part if total is None else total + part
        return total

    bias3 = bias_ref[2]
    columns = [
        jnp.maximum(
            column_sum(c, 1)
            + up(column_sum(c, 0), 1, tgt_cols)
            + down(column_sum(c, 2), 1, tgt_cols)
            + bias3,
            0.0,
        )
        for c in range(inner)
    ]
    scores = jnp.stack(columns, axis=0).swapaxes(0, 1)
    for n in range(cells):
        for b in range(LANES // tgt_cols):
            out_ref[n // rows_b, n % rows_b, b * inner : (b + 1) * inner] = scores[
                n, :, b * tgt_cols : (b + 1) * tgt_cols
            ].astype(jnp.bfloat16)


VMEM = pl.BlockSpec(memory_space=pltpu.VMEM)
SMEM = pl.BlockSpec(memory_space=pltpu.SMEM)


def one_pair(source, target, conv_one, bias_one, conv_two, bias_two, conv_three, bias_three):
    rows_a, src_cols, _ = source.shape
    rows_b, tgt_cols, _ = target.shape
    channels = conv_two.shape[-1]
    blocks = LANES // tgt_cols
    inner = src_cols // blocks
    assert 2 * inner == channels and LANES % tgt_cols == 0
    assert rows_a % 2 == 0 and rows_b % 2 == 0 and min(rows_a, rows_b) >= HALO

    left, left_masks = xor_blocks(source.reshape(rows_a * src_cols, -1), "tgt")
    right, right_masks = xor_blocks(target.reshape(rows_b * tgt_cols, -1), "src")
    left, left_masks, left_axis = wide_blocks(left, left_masks, "tgt")
    right, right_masks, right_axis = wide_blocks(right, right_masks, "src")

    taps = TAPS**4
    w3_cols = (rows_a + 2) * LANES
    w3_rows = TAPS * TAPS * rows_a * rows_b
    w1_cols = -(-(len(first_tiles()) * 2 * inner) // LANES) * LANES
    biases, w1, w2, w3 = pl.pallas_call(
        partial(weights_kernel, inner=inner, rows_a=rows_a, rows_b=rows_b),
        out_shape=(
            jax.ShapeDtypeStruct((TAPS, channels, LANES), jnp.float32),
            jax.ShapeDtypeStruct((2 * LANES, w1_cols), jnp.bfloat16),
            jax.ShapeDtypeStruct((TAPS * 4 * channels, TAPS * 2 * LANES), jnp.bfloat16),
            jax.ShapeDtypeStruct((w3_rows, w3_cols), jnp.bfloat16),
        ),
        in_specs=[SMEM] * 3 + [VMEM] * 3,
        out_specs=(VMEM,) * 4,
        scratch_shapes=[pltpu.VMEM((w3_rows, w3_cols), jnp.float32)],
        cost_estimate=pl.CostEstimate(flops=2_000_000_000, bytes_accessed=1_000_000, transcendentals=0),
        compiler_params=pltpu.CompilerParams(vmem_limit_bytes=8 << 20),
        name="weights",
    )(
        bias_one,
        bias_two,
        bias_three,
        conv_one.reshape(-1, TAPS, channels),
        conv_two.reshape(taps, channels, channels).swapaxes(1, 2).reshape(taps * channels, channels),
        conv_three.reshape(-1, TAPS, channels),
    )

    def held(pieces):
        return pltpu.VMEM((sum(p.shape[0] for p in pieces), *pieces[0].shape[1:]), jnp.bfloat16)

    edge = jax.ShapeDtypeStruct((HALO, rows_b, inner, LANES), jnp.bfloat16)
    own, low_edge, high_edge = pl.pallas_call(
        partial(
            volume_kernel,
            masks=(left_masks, right_masks),
            axes=(left_axis, right_axis),
            src_cols=src_cols,
            tgt_cols=tgt_cols,
        ),
        out_shape=(jax.ShapeDtypeStruct((rows_a, rows_b, inner, LANES), jnp.bfloat16), edge, edge),
        in_specs=[VMEM] * (len(left) + len(right)),
        out_specs=(VMEM,) * 3,
        scratch_shapes=[held(left), held(right)],
        compiler_params=pltpu.CompilerParams(vmem_limit_bytes=8 << 20),
        name="volume",
    )(*left, *right)

    low_a, high_a = swap_edges(low_edge, high_edge, "src")
    tall = [low_a, own, high_a]
    low_edge = jnp.concatenate([x[:, :HALO] for x in tall], axis=0)
    high_edge = jnp.concatenate([x[:, rows_b - HALO :] for x in tall], axis=0)
    low_b, high_b = swap_edges(low_edge, high_edge, "tgt")
    ext_a, ext_b = rows_a + 2 * HALO, rows_b + 2 * HALO
    return pl.pallas_call(
        partial(
            layers_kernel,
            sizes=(lax.axis_size("src"), lax.axis_size("tgt")),
            tgt_cols=tgt_cols,
            inner=inner,
            channels=channels,
        ),
        out_shape=jax.ShapeDtypeStruct((rows_a, rows_b, src_cols, tgt_cols), jnp.bfloat16),
        in_specs=[VMEM] * 9,
        out_specs=VMEM,
        scratch_shapes=[
            pltpu.VMEM((TAPS, ext_a, ext_b, 2 * inner, LANES), jnp.bfloat16),
            pltpu.VMEM((ext_a - 2, ext_b - 2, (inner + 2) * channels, LANES), jnp.bfloat16),
            pltpu.VMEM((ext_a - 4, ext_b - 4, inner * channels, LANES), jnp.bfloat16),
        ],
        compiler_params=pltpu.CompilerParams(vmem_limit_bytes=20 << 20),
        name="layers",
    )(biases, own, low_a, high_a, low_b, high_b, w1, w2, w3)


def local(source_feats, target_feats, *params):
    return jnp.stack(
        [one_pair(source_feats[p], target_feats[p], *params) for p in range(source_feats.shape[0])]
    )


def solution(mesh):
    return jax.shard_map(
        local,
        mesh=mesh,
        in_specs=(
            P(None, "src", None, "tgt"),
            P(None, "tgt", None, "src"),
            P(),
            P(),
            P(),
            P(),
            P(),
            P(),
        ),
        out_specs=P(None, "src", "tgt", None, None),
        check_vma=False,
    )
```
